128 devices in a mesh: gx: 8 (over y, core), gy: 16 (over x, z).
Axes of the slice: x: 4, y: 4, z: 4, core: 2. Of those that a mesh axis runs over, the one named last changes fastest.
Arguments:
- right_side: float32 [256, 512, 512], P('gx', 'gy'), as said below
- start_guess: float32 [256, 512, 512], P('gx', 'gy'), may hold values from -3 to 3
- conductivity: float32 [256, 512, 512], P('gx', 'gy'), may hold values from 0.5 to 8
Outputs:
- solution_field: float32 [256, 512, 512], P('gx', 'gy')
- estimate: float32 [], replicated
The draws below stay inside these ranges and needn't reach their ends.
Inputs may be any that keep to these rules, and one draw needn't show every extreme that they name: `right_side`: A smoothly varying positive scale times noise, which may have a nonzero mean.
All inputs are finite; a program needn't handle non-finite values.
Results may differ from the reference program's by a relative error of at most 0.0003.
Values sent between devices are 32-bit elements; how exact they have to be, the bound alone decides.
A program may use at most 64 MiB of HBM per device.

```python
import math
import jax
import jax.numpy as jnp
from jax import lax

CZ = 512
M = 3
NX = 256
NY = 512


def draw_right_side(key, part):
    noise = jax.random.normal(jax.random.fold_in(key, 7), (NX, NY, CZ), jnp.float32)
    first = (jnp.arange(NX, dtype=jnp.float32) / NX)[:, None, None]
    second = (jnp.arange(NY, dtype=jnp.float32) / NY)[None, :, None]
    scale = (0.5 + first) * (0.5 + second)
    return scale * noise


def block_levels(rng, shape, split, least, high):
    loudness, own = 1.0, jax.random.fold_in(rng, 6)
    for axis_at, blocks in split:
        steps = jnp.exp(jax.random.uniform(jax.random.fold_in(own, axis_at), (blocks,), jnp.float32, least / len(split), high / len(split)))
        loudness = loudness * jnp.repeat(steps, shape[axis_at] // blocks).reshape([-1 if axis == axis_at else 1 for axis in range(len(shape))])
    return loudness


def normal_values(rng, shape, deviation, bound, split=(), kind=jnp.bfloat16):
    drawn = jax.random.normal(rng, shape, jnp.float32) * deviation
    if len(split) > 0:
        drawn = block_levels(rng, shape, split, -0.22, 0.18) * drawn
    return jnp.clip(drawn, min=-bound, max=bound).astype(kind)


def setup_inputs(seed: int = 0) -> dict:
    keys = jax.random.split(jax.random.key(seed), 4)
    return {
        "right_side": draw_right_side(jax.random.fold_in(keys[3], 71), 0),
        "start_guess": normal_values(keys[1], (NX, NY, CZ), 0.5, 3.0, ((0, 8), (1, 16)), jnp.float32),
        "conductivity": jnp.clip(jnp.exp(math.log(8.0) - 2.7725887 * jax.random.uniform(keys[2], (NX, NY, CZ), jnp.float32) ** block_levels(keys[2], (NX, NY, CZ), ((0, 8), (1, 16)), -0.2, 0.2)), 0.5, 8.0),
    }


def shifted(padded, which, sign):
    starts = [1, 1, 1]
    starts[which] = 1 + sign
    limits = [starts[dim] + padded.shape[dim] - 2 for dim in range(3)]
    return lax.slice(padded, starts, limits)

def stencil(padded, kappa_pad):
    centre = shifted(padded, 0, 0)
    middle = shifted(kappa_pad, 0, 0)
    result = jnp.zeros_like(centre)
    for which in range(3):
        for sign in (-1, 1):
            result = result + 0.5 * (middle + shifted(kappa_pad, which, sign)) * (centre - shifted(padded, which, sign))
    return result

def least_squares(columns, beta):
    count = len(columns)
    rhs_vals = [beta] + [jnp.float32(0.0)] * count
    cosines = []
    sines = []
    upper = []
    for column in range(count):
        entries = list(columns[column])
        for earlier in range(column):
            first = entries[earlier]
            second = entries[earlier + 1]
            entries[earlier] = cosines[earlier] * first + sines[earlier] * second
            entries[earlier + 1] = -sines[earlier] * first + cosines[earlier] * second
        first = entries[column]
        second = entries[column + 1]
        radius = jnp.sqrt(first * first + second * second)
        cosines.append(first / radius)
        sines.append(second / radius)
        entries[column] = radius
        rhs_vals[column + 1] = -sines[column] * rhs_vals[column]
        rhs_vals[column] = cosines[column] * rhs_vals[column]
        upper.append(entries[:column + 1])
    coeffs = [None] * count
    for row in reversed(range(count)):
        value = rhs_vals[row]
        for later in range(row + 1, count):
            value = value - upper[later][row] * coeffs[later]
        coeffs[row] = value / upper[row][row]
    return (coeffs, jnp.abs(rhs_vals[count]))

def reference(right_side, start_guess, conductivity):
    kappa_pad = jnp.pad(conductivity, 1)
    start = right_side - stencil(jnp.pad(start_guess, 1), kappa_pad)
    beta = jnp.sqrt(jnp.sum(start * start))
    basis = [start / beta]
    columns = []
    for column in range(M):
        vector = stencil(jnp.pad(basis[column], 1), kappa_pad)
        entries = []
        for earlier in range(column + 1):
            coeff = jnp.sum(vector * basis[earlier])
            vector = vector - coeff * basis[earlier]
            entries.append(coeff)
        length = jnp.sqrt(jnp.sum(vector * vector))
        entries.append(length)
        columns.append(entries)
        basis.append(vector / length)
    coeffs, estimate = least_squares(columns, beta)
    solution_field = start_guess
    for column in range(M):
        solution_field = solution_field + coeffs[column] * basis[column]
    return (solution_field, estimate)
```

```python
import functools

import jax
import jax.numpy as jnp
from jax import lax
from jax.experimental import pallas as pl
from jax.experimental.pallas import tpu as pltpu
from jax.sharding import PartitionSpec as P

MESH = pl.DeviceIdType.MESH
F32 = jnp.float32
SCALE = 64.0
HALF = 0.5 / SCALE
R0, R1 = 8, 136
PLANES, ROWS = 34, 144


def renorm(a, b):
    s = a + b
    return s, b - (s - a)


def two_sum(a, b):
    s = a + b
    t = s - a
    return s, (a - (s - t)) + (b - t)


def split(a):
    t = 4097.0 * a
    high = t - (t - a)
    return high, a - high


def two_prod(a, b):
    p = a * b
    (ah, al), (bh, bl) = split(a), split(b)
    return p, ((ah * bh - p) + ah * bl + al * bh) + al * bl


def add(a, b):
    s, e = two_sum(a[0], b[0])
    return renorm(s, e + (a[1] + b[1]))


def sub(a, b):
    return add(a, (-b[0], -b[1]))


def mul(a, b):
    p, e = two_prod(a[0], b[0])
    return renorm(p, e + (a[0] * b[1] + a[1] * b[0]))


def div(a, b):
    q = a[0] / b[0]
    p, e = two_prod(q, b[0])
    return renorm(q, (((a[0] - p) - e) + (a[1] - q * b[1])) / b[0])


def normal_equations(m):
    l21, l31 = div(m[3], m[2]), div(m[4], m[2])
    d2 = sub(m[4], mul(l21, m[3]))
    e2 = sub(m[5], mul(l21, m[4]))
    l32 = div(e2, d2)
    d3 = sub(sub(m[6], mul(l31, m[4])), mul(l32, e2))
    c1 = m[1]
    c2 = sub(m[2], mul(l21, c1))
    c3 = sub(sub(m[3], mul(l31, c1)), mul(l32, c2))
    q1, q2, q3 = div(c1, m[2]), div(c2, d2), div(c3, d3)
    y3 = q3
    y2 = sub(q2, mul(l32, y3))
    y1 = sub(sub(q1, mul(l21, y2)), mul(l31, y3))
    rest = sub(sub(sub(m[0], mul(c1, q1)), mul(c2, q2)), mul(c3, q3))
    return tuple(y[0] / SCALE for y in (y1, y2, y3)), rest[0]


def directions(gx, gy, ngx, ngy):
    return (
        ("gy", 1, gy < ngy - 1, gy > 0),
        ("gy", -1, gy > 0, gy < ngy - 1),
        ("gx", 1, gx < ngx - 1, gx > 0),
        ("gx", -1, gx > 0, gx < ngx - 1),
    )


def face(ref, axis, step):
    if axis == "gx":
        return ref.at[32 if step > 0 else 1, R0:R1, :]
    return ref.at[1:33, (R1 - 4 if step > 0 else R0) : (R1 if step > 0 else R0 + 4), :]


def halo(ref, axis, step):
    if axis == "gx":
        return ref.at[0 if step > 0 else 33, R0:R1, :]
    return ref.at[1:33, (R0 - 4 if step > 0 else R1) : (R0 if step > 0 else R1 + 4), :]


def kernel(
    ngx, ngy,
    rhs_hbm, x0_hbm, k_hbm, sol_ref, est_ref,
    kp, up, rp, v1, v2, rb, wx, wy, wzm, wzp, dg, row, gath,
    load_sem, send_sem, recv_sem, gsend, grecv, ready,
):
    gx, gy = lax.axis_index("gx"), lax.axis_index("gy")
    count = ngx * ngy
    loads = []
    for i, (src, dst) in enumerate(((k_hbm, kp), (x0_hbm, up))):
        view = dst.reshape(PLANES, ROWS // 4, 4, 128)
        for q in range(4):
            loads.append(
                pltpu.make_async_copy(
                    src.at[:, :, q * 128 : (q + 1) * 128], view.at[1:33, 2:34, q, :], load_sem.at[i, q]
                )
            )
    view = rb.reshape(32, 32, 4, 128)
    for q in range(4):
        loads.append(
            pltpu.make_async_copy(rhs_hbm.at[:, :, q * 128 : (q + 1) * 128], view.at[:, :, q, :], load_sem.at[2, q])
        )
    for copy in loads:
        copy.start()

    barrier = pltpu.get_barrier_semaphore()
    for d in range(1, ngx):
        pl.semaphore_signal(barrier, inc=1, device_id=(lax.rem(gx + d, ngx), gy), device_id_type=MESH)
    for d in range(1, ngy):
        pl.semaphore_signal(barrier, inc=1, device_id=(gx, lax.rem(gy + d, ngy)), device_id_type=MESH)

    dirs = directions(gx, gy, ngx, ngy)
    fields = (kp, up, rp, v1, v2)
    zplane = jnp.zeros((R1 - R0, 128), F32)
    zrow = jnp.zeros((4, 128), F32)

    @pl.when(gx == 0)
    def _():
        for f in fields:
            f[0, R0:R1, :] = zplane

    @pl.when(gx == ngx - 1)
    def _():
        for f in fields:
            f[33, R0:R1, :] = zplane

    for at, edge in ((R0 - 4, 0), (R1, ngy - 1)):

        @pl.when(gy == edge)
        def _():
            def fill(x, c):
                for f in fields:
                    f[x, at : at + 4, :] = zrow
                return c

            lax.fori_loop(1, 33, fill, 0)

    def exchange(e, f, axes=("gx", "gy")):
        for i, (axis, step, to, _) in enumerate(dirs):
            if axis in axes:

                @pl.when(to)
                def _():
                    me = gx if axis == "gx" else gy
                    pltpu.make_async_remote_copy(
                        src_ref=face(f, axis, step), dst_ref=halo(f, axis, step),
                        send_sem=send_sem.at[e, i], recv_sem=recv_sem.at[e, i],
                        device_id={axis: me + step}, device_id_type=MESH,
                    ).start()

    def descriptor(e, f, i):
        axis, step = dirs[i][:2]
        return pltpu.make_async_remote_copy(
            src_ref=face(f, axis, step), dst_ref=halo(f, axis, step),
            send_sem=send_sem.at[e, i], recv_sem=recv_sem.at[e, i],
            device_id={axis: gx if axis == "gx" else gy}, device_id_type=MESH,
        )

    def arrived(e, f, axes):
        for i, (axis, _, _, come) in enumerate(dirs):
            if axis in axes:

                @pl.when(come)
                def _():
                    descriptor(e, f, i).wait_recv()

    def sent(e, f):
        for i, (_, _, to, _) in enumerate(dirs):

            @pl.when(to)
            def _():
                descriptor(e, f, i).wait_send()

    for copy in loads[:4]:
        copy.wait()
    pl.semaphore_wait(barrier, ngx + ngy - 2)
    exchange(0, kp)
    for copy in loads[4:8]:
        copy.wait()
    exchange(1, up)
    for d in range(1, ngx):
        pl.semaphore_signal(ready, inc=1, device_id=(lax.rem(gx + d, ngx), gy), device_id_type=MESH)

    lane = lax.broadcasted_iota(jnp.int32, (8, 128), 1)
    zhi = lax.rem(lax.broadcasted_iota(jnp.int32, (8, 128), 0), 4)
    first_lane, last_lane = lane == 0, lane == 127
    z_first = jnp.logical_and(first_lane, zhi == 0)
    z_last = jnp.logical_and(last_lane, zhi == 3)

    def z_up(f, x, r, centre):
        return pltpu.roll(jnp.where(first_lane, f[x, r + 1 : r + 9, :], centre), 127, 1)

    def z_down(f, x, r, centre):
        return pltpu.roll(jnp.where(last_lane, f[x, r - 1 : r + 7, :], centre), 1, 1)

    def weights_x(i, chunks):
        for r in chunks:
            wx[i, r - R0 : r - R0 + 8, :] = HALF * (kp[i, r : r + 8, :] + kp[i + 1, r : r + 8, :])

    def weights_y(x, r, n=8):
        wy[x, r : r + n, :] = HALF * (kp[x, r : r + n, :] + kp[x, r + 4 : r + 4 + n, :])

    def weights_z(x, r):
        centre = kp[x, r : r + 8, :]
        above = jnp.where(first_lane, pltpu.roll(centre, 7, 0), centre)
        below = jnp.where(last_lane, pltpu.roll(centre, 1, 0), centre)
        up_w = HALF * (centre + jnp.where(z_last, 0.0, pltpu.roll(above, 127, 1)))
        down_w = HALF * (centre + jnp.where(z_first, 0.0, pltpu.roll(below, 1, 1)))
        dg[x, r - R0 : r - R0 + 8, :] = up_w + down_w
        wzp[x, r - R0 : r - R0 + 8, :] = jnp.where(z_last, 0.0, up_w)
        wzm[x, r - R0 : r - R0 + 8, :] = jnp.where(z_first, 0.0, down_w)

    def add_diagonal(x, r):
        q = r - R0
        dg[x, q : q + 8, :] = dg[x, q : q + 8, :] + (
            (wx[x - 1, q : q + 8, :] + wx[x, q : q + 8, :]) + (wy[x, r - 4 : r + 4, :] + wy[x, r : r + 8, :])
        )

    def apply(f, x, r):
        q = r - R0
        centre = f[x, r : r + 8, :]
        out = dg[x, q : q + 8, :] * centre
        out = out - wx[x - 1, q : q + 8, :] * f[x - 1, r : r + 8, :]
        out = out - wx[x, q : q + 8, :] * f[x + 1, r : r + 8, :]
        out = out - wy[x, r - 4 : r + 4, :] * f[x, r - 4 : r + 4, :]
        out = out - wy[x, r : r + 8, :] * f[x, r + 4 : r + 12, :]
        out = out - wzm[x, q : q + 8, :] * z_down(f, x, r, centre)
        out = out - wzp[x, q : q + 8, :] * z_up(f, x, r, centre)
        return centre, out

    inner = tuple(range(R0 + 8, R1 - 8, 8))
    whole = tuple(range(R0, R1, 8))
    ends = (R0, R1 - 8)

    def over(planes, body, carry):
        if isinstance(planes, range):
            return lax.fori_loop(planes.start, planes.stop, body, carry)
        for x in planes:
            carry = body(x, carry)
        return carry

    def residual(planes, chunks, acc):
        def body(x, acc):
            for r in chunks:
                _, out = apply(up, x, r)
                out = rb[x - 1, r - R0 : r - R0 + 8, :] - SCALE * out
                rp[x, r : r + 8, :] = out
                acc = acc + out * out
            return acc

        return over(planes, body, acc)

    def power(f, w, planes, chunks, acc):
        def body(x, acc):
            cross, square = acc
            for r in chunks:
                centre, out = apply(f, x, r)
                if w is not None:
                    w[x, r : r + 8, :] = out
                cross, square = cross + centre * out, square + out * out
            return cross, square

        return over(planes, body, acc)

    def body(x, c):
        weights_x(x, whole)
        for r in whole[:-1]:
            weights_y(x, r)
        weights_y(x, R1 - 8, 4)
        for r in whole:
            weights_z(x, r)
        for r in inner:
            add_diagonal(x, r)
        return c

    weights_x(1, whole)
    lax.fori_loop(2, 32, body, 0)
    for x in (1, 32):
        for r in whole[:-1]:
            weights_y(x, r)
        weights_y(x, R1 - 8, 4)
        for r in whole:
            weights_z(x, r)
    for copy in loads[8:]:
        copy.wait()
    zero = jnp.zeros((8, 128), F32)
    m0 = residual(range(2, 32), inner, zero)
    arrived(0, kp, ("gx",))
    weights_x(0, whole)
    weights_x(32, whole)
    for x in (1, 32):
        for r in inner:
            add_diagonal(x, r)
    arrived(1, up, ("gx",))
    m0 = residual((1, 32), inner, m0)
    arrived(0, kp, ("gy",))

    def body(x, c):
        weights_y(x, R0 - 4, 4)
        weights_y(x, R1 - 4, 4)
        for r in ends:
            add_diagonal(x, r)
        return c

    lax.fori_loop(1, 33, body, 0)
    arrived(1, up, ("gy",))
    m0 = residual(range(1, 33), ends, m0)

    moments = [m0]
    for e, (f, w) in enumerate(((rp, v1), (v1, v2), (v2, None)), start=2):
        exchange(e, f)
        acc = power(f, w, range(2, 32), inner, (zero, zero))
        arrived(e, f, ("gx",))
        acc = power(f, w, (1, 32), inner, acc)
        arrived(e, f, ("gy",))
        acc = power(f, w, range(1, 33), ends, acc)
        moments.extend(acc)

    sub = lax.broadcasted_iota(jnp.int32, (8, 128), 0)
    stacked = zero
    for k, m in enumerate(moments):
        stacked = jnp.where(sub == k, jnp.sum(m, axis=0, keepdims=True), stacked)
    sums = jnp.sum(stacked, axis=1, keepdims=True)
    own = jnp.sum(jnp.where(lane == sub, sums, 0.0), axis=0, keepdims=True)
    place = gx * ngy + gy
    row[...] = own
    gath[pl.ds(place, 1), :] = own
    pl.semaphore_wait(ready, ngx - 1)

    def send(d, c):
        pltpu.make_async_remote_copy(
            src_ref=row, dst_ref=gath.at[pl.ds(place, 1), :], send_sem=gsend, recv_sem=grecv,
            device_id=(lax.rem(gx + d // ngy, ngx), lax.rem(gy + lax.rem(d, ngy), ngy)), device_id_type=MESH,
        ).start()
        return c

    lax.fori_loop(1, count, send, 0)
    every = pltpu.make_async_remote_copy(
        src_ref=gath.at[0 : count - 1, :], dst_ref=gath.at[0 : count - 1, :], send_sem=gsend, recv_sem=grecv,
        device_id=(gx, gy), device_id_type=MESH,
    )
    every.wait_recv()
    table = gath[...]
    bound = 2.0 * jnp.sum(jnp.abs(table), axis=0, keepdims=True)
    upper = (table + bound) - bound
    high = jnp.sum(upper, axis=0, keepdims=True)
    low = jnp.sum(table - upper, axis=0, keepdims=True)
    lane1 = lax.broadcasted_iota(jnp.int32, (1, 128), 1)

    def pick(v, k):
        return jnp.sum(jnp.where(lane1 == k, v, 0.0), axis=1, keepdims=True)

    m = [renorm(pick(high, k), pick(low, k)) for k in range(7)]
    (y1, y2, y3), rest = normal_equations(m)
    est_ref[...] = jnp.broadcast_to(jnp.sqrt(jnp.maximum(rest, 0.0)), (1, 128))
    y1, y2, y3 = (jnp.broadcast_to(y, (8, 128)) for y in (y1, y2, y3))

    def body(x, c):
        for r in whole:
            s = slice(r, r + 8)
            sol_ref[x - 1, r - R0 : r - R0 + 8, :] = up[x, s, :] + (
                y1 * rp[x, s, :] + (y2 * v1[x, s, :] + y3 * v2[x, s, :])
            )
        return c

    lax.fori_loop(1, 33, body, 0)
    every.wait_send()
    for e, f in enumerate((kp, up, rp, v1, v2)):
        sent(e, f)


def local(ngx, ngy, right_side, start_guess, conductivity):
    field = pltpu.VMEM((PLANES, ROWS, 128), F32)
    block = pltpu.VMEM((32, 128, 128), F32)
    sem = pltpu.SemaphoreType
    sol, est = pl.pallas_call(
        functools.partial(kernel, ngx, ngy),
        out_shape=(jax.ShapeDtypeStruct((32, 128, 128), F32), jax.ShapeDtypeStruct((1, 128), F32)),
        in_specs=[pl.BlockSpec(memory_space=pl.ANY)] * 3,
        out_specs=(pl.BlockSpec(memory_space=pltpu.VMEM), pl.BlockSpec(memory_space=pltpu.VMEM)),
        scratch_shapes=[field] * 5 + [
            block,
            pltpu.VMEM((33, 128, 128), F32),
            pltpu.VMEM((33, ROWS, 128), F32),
            pltpu.VMEM((33, 128, 128), F32),
            pltpu.VMEM((33, 128, 128), F32),
            pltpu.VMEM((33, 128, 128), F32),
            pltpu.VMEM((1, 128), F32),
            pltpu.VMEM((ngx * ngy, 128), F32),
            sem.DMA((3, 4)), sem.DMA((5, 4)), sem.DMA((5, 4)), sem.DMA, sem.DMA, sem.REGULAR,
        ],
        compiler_params=pltpu.CompilerParams(
            collective_id=0, has_side_effects=True, vmem_limit_bytes=62 * 2**20
        ),
    )(right_side, start_guess, conductivity)
    return sol.reshape(32, 32, 512), est[0, 0]


def solution(mesh):
    return jax.shard_map(
        functools.partial(local, mesh.shape["gx"], mesh.shape["gy"]),
        mesh=mesh,
        in_specs=(P("gx", "gy", None),) * 3,
        out_specs=(P("gx", "gy", None), P()),
        check_vma=False,
    )
```

```python
import functools

import jax
import jax.numpy as jnp
from jax import lax
from jax.experimental import pallas as pl
from jax.experimental.pallas import tpu as pltpu
from jax.sharding import PartitionSpec as P

MESH = pl.DeviceIdType.MESH
F32 = jnp.float32
SCALE = 64.0
HALF = 0.5 / SCALE
R0, R1 = 8, 136
PLANES, ROWS = 34, 144


def renorm(a, b):
    s = a + b
    return s, b - (s - a)


def two_sum(a, b):
    s = a + b
    t = s - a
    return s, (a - (s - t)) + (b - t)


def split(a):
    t = 4097.0 * a
    high = t - (t - a)
    return high, a - high


def two_prod(a, b):
    p = a * b
    (ah, al), (bh, bl) = split(a), split(b)
    return p, ((ah * bh - p) + ah * bl + al * bh) + al * bl


def add(a, b):
    s, e = two_sum(a[0], b[0])
    return renorm(s, e + (a[1] + b[1]))


def sub(a, b):
    return add(a, (-b[0], -b[1]))


def mul(a, b):
    p, e = two_prod(a[0], b[0])
    return renorm(p, e + (a[0] * b[1] + a[1] * b[0]))


def div(a, b):
    q = a[0] / b[0]
    p, e = two_prod(q, b[0])
    return renorm(q, (((a[0] - p) - e) + (a[1] - q * b[1])) / b[0])


def normal_equations(m):
    l21, l31 = div(m[3], m[2]), div(m[4], m[2])
    d2 = sub(m[4], mul(l21, m[3]))
    e2 = sub(m[5], mul(l21, m[4]))
    l32 = div(e2, d2)
    d3 = sub(sub(m[6], mul(l31, m[4])), mul(l32, e2))
    c1 = m[1]
    c2 = sub(m[2], mul(l21, c1))
    c3 = sub(sub(m[3], mul(l31, c1)), mul(l32, c2))
    q1, q2, q3 = div(c1, m[2]), div(c2, d2), div(c3, d3)
    y3 = q3
    y2 = sub(q2, mul(l32, y3))
    y1 = sub(sub(q1, mul(l21, y2)), mul(l31, y3))
    rest = sub(sub(sub(m[0], mul(c1, q1)), mul(c2, q2)), mul(c3, q3))
    return tuple(y[0] / SCALE for y in (y1, y2, y3)), rest[0]


def directions(gx, gy, ngx, ngy):
    return (
        ("gy", 1, gy < ngy - 1, gy > 0),
        ("gy", -1, gy > 0, gy < ngy - 1),
        ("gx", 1, gx < ngx - 1, gx > 0),
        ("gx", -1, gx > 0, gx < ngx - 1),
    )


def far_first(ngx, ngy):
    def ring(d):
        return min(d % 4, -d % 4)

    offsets = [(dx, dy) for dx in range(ngx) for dy in range(ngy) if dx or dy]
    return sorted(offsets, key=lambda o: -(ring(o[0] // 2) + ring(o[1] // 4) + ring(o[1] % 4)))


def face(ref, axis, step):
    if axis == "gx":
        return ref.at[32 if step > 0 else 1, R0:R1, :]
    return ref.at[1:33, (R1 - 4 if step > 0 else R0) : (R1 if step > 0 else R0 + 4), :]


def halo(ref, axis, step):
    if axis == "gx":
        return ref.at[0 if step > 0 else 33, R0:R1, :]
    return ref.at[1:33, (R0 - 4 if step > 0 else R1) : (R0 if step > 0 else R1 + 4), :]


def kernel(
    ngx, ngy,
    rhs_hbm, x0_hbm, k_hbm, sol_ref, est_ref,
    kp, up, rp, v1, v2, rb, wx, wy, wzm, wzp, dg, row, gath,
    load_sem, send_sem, recv_sem, gsend, grecv, ready,
):
    gx, gy = lax.axis_index("gx"), lax.axis_index("gy")
    count = ngx * ngy
    loads = []
    for i, (src, dst) in enumerate(((k_hbm, kp), (x0_hbm, up))):
        view = dst.reshape(PLANES, ROWS // 4, 4, 128)
        for q in range(4):
            loads.append(
                pltpu.make_async_copy(
                    src.at[:, :, q * 128 : (q + 1) * 128], view.at[1:33, 2:34, q, :], load_sem.at[i, q]
                )
            )
    view = rb.reshape(32, 32, 4, 128)
    for q in range(4):
        loads.append(
            pltpu.make_async_copy(rhs_hbm.at[:, :, q * 128 : (q + 1) * 128], view.at[:, :, q, :], load_sem.at[2, q])
        )
    for copy in loads:
        copy.start()

    barrier = pltpu.get_barrier_semaphore()
    for d in range(1, ngx):
        pl.semaphore_signal(barrier, inc=1, device_id=(lax.rem(gx + d, ngx), gy), device_id_type=MESH)
    for d in range(1, ngy):
        pl.semaphore_signal(barrier, inc=1, device_id=(gx, lax.rem(gy + d, ngy)), device_id_type=MESH)

    dirs = directions(gx, gy, ngx, ngy)
    fields = (kp, up, rp, v1, v2)
    zplane = jnp.zeros((R1 - R0, 128), F32)
    zrow = jnp.zeros((4, 128), F32)

    @pl.when(gx == 0)
    def _():
        for f in fields:
            f[0, R0:R1, :] = zplane

    @pl.when(gx == ngx - 1)
    def _():
        for f in fields:
            f[33, R0:R1, :] = zplane

    for at, edge in ((R0 - 4, 0), (R1, ngy - 1)):

        @pl.when(gy == edge)
        def _():
            def fill(x, c):
                for f in fields:
                    f[x, at : at + 4, :] = zrow
                return c

            lax.fori_loop(1, 33, fill, 0)

    def exchange(e, f, axes=("gx", "gy")):
        for i, (axis, step, to, _) in enumerate(dirs):
            if axis in axes:

                @pl.when(to)
                def _():
                    me = gx if axis == "gx" else gy
                    pltpu.make_async_remote_copy(
                        src_ref=face(f, axis, step), dst_ref=halo(f, axis, step),
                        send_sem=send_sem.at[e, i], recv_sem=recv_sem.at[e, i],
                        device_id={axis: me + step}, device_id_type=MESH,
                    ).start()

    def descriptor(e, f, i):
        axis, step = dirs[i][:2]
        return pltpu.make_async_remote_copy(
            src_ref=face(f, axis, step), dst_ref=halo(f, axis, step),
            send_sem=send_sem.at[e, i], recv_sem=recv_sem.at[e, i],
            device_id={axis: gx if axis == "gx" else gy}, device_id_type=MESH,
        )

    def arrived(e, f, axes):
        for i, (axis, _, _, come) in enumerate(dirs):
            if axis in axes:

                @pl.when(come)
                def _():
                    descriptor(e, f, i).wait_recv()

    def sent(e, f):
        for i, (_, _, to, _) in enumerate(dirs):

            @pl.when(to)
            def _():
                descriptor(e, f, i).wait_send()

    with jax.named_scope("load_k"):
        for copy in loads[:4]:
            copy.wait()
    with jax.named_scope("barrier"):
        pl.semaphore_wait(barrier, ngx + ngy - 2)
        exchange(0, kp)
        for copy in loads[4:8]:
            copy.wait()
        exchange(1, up)
    for d in range(1, ngx):
        pl.semaphore_signal(ready, inc=1, device_id=(lax.rem(gx + d, ngx), gy), device_id_type=MESH)

    lane = lax.broadcasted_iota(jnp.int32, (8, 128), 1)
    zhi = lax.rem(lax.broadcasted_iota(jnp.int32, (8, 128), 0), 4)
    first_lane, last_lane = lane == 0, lane == 127
    z_first = jnp.logical_and(first_lane, zhi == 0)
    z_last = jnp.logical_and(last_lane, zhi == 3)

    def z_up(f, x, r, centre):
        return pltpu.roll(jnp.where(first_lane, f[x, r + 1 : r + 9, :], centre), 127, 1)

    def z_down(f, x, r, centre):
        return pltpu.roll(jnp.where(last_lane, f[x, r - 1 : r + 7, :], centre), 1, 1)

    def weights_x(i, chunks):
        for r in chunks:
            wx[i, r - R0 : r - R0 + 8, :] = HALF * (kp[i, r : r + 8, :] + kp[i + 1, r : r + 8, :])

    def weights_y(x, r, n=8):
        wy[x, r : r + n, :] = HALF * (kp[x, r : r + n, :] + kp[x, r + 4 : r + 4 + n, :])

    def weights_z(x, r):
        centre = kp[x, r : r + 8, :]
        above = jnp.where(first_lane, pltpu.roll(centre, 7, 0), centre)
        below = jnp.where(last_lane, pltpu.roll(centre, 1, 0), centre)
        up_w = HALF * (centre + jnp.where(z_last, 0.0, pltpu.roll(above, 127, 1)))
        down_w = HALF * (centre + jnp.where(z_first, 0.0, pltpu.roll(below, 1, 1)))
        dg[x, r - R0 : r - R0 + 8, :] = up_w + down_w
        wzp[x, r - R0 : r - R0 + 8, :] = jnp.where(z_last, 0.0, up_w)
        wzm[x, r - R0 : r - R0 + 8, :] = jnp.where(z_first, 0.0, down_w)

    def add_diagonal(x, r):
        q = r - R0
        dg[x, q : q + 8, :] = dg[x, q : q + 8, :] + (
            (wx[x - 1, q : q + 8, :] + wx[x, q : q + 8, :]) + (wy[x, r - 4 : r + 4, :] + wy[x, r : r + 8, :])
        )

    def apply(f, x, r):
        q = r - R0
        centre = f[x, r : r + 8, :]
        out = dg[x, q : q + 8, :] * centre
        out = out - wx[x - 1, q : q + 8, :] * f[x - 1, r : r + 8, :]
        out = out - wx[x, q : q + 8, :] * f[x + 1, r : r + 8, :]
        out = out - wy[x, r - 4 : r + 4, :] * f[x, r - 4 : r + 4, :]
        out = out - wy[x, r : r + 8, :] * f[x, r + 4 : r + 12, :]
        out = out - wzm[x, q : q + 8, :] * z_down(f, x, r, centre)
        out = out - wzp[x, q : q + 8, :] * z_up(f, x, r, centre)
        return centre, out

    inner = tuple(range(R0 + 8, R1 - 8, 8))
    whole = tuple(range(R0, R1, 8))
    ends = (R0, R1 - 8)

    def over(planes, body, carry, unroll=1):
        if not isinstance(planes, range):
            for x in planes:
                carry = body(x, carry)
            return carry
        first, steps = planes.start, len(planes) // unroll

        def several(i, carry):
            for u in range(unroll):
                carry = body(first + i * unroll + u, carry)
            return carry

        return lax.fori_loop(0, steps, several, carry)

    def residual(planes, chunks, acc):
        def body(x, acc):
            for r in chunks:
                _, out = apply(up, x, r)
                out = rb[x - 1, r - R0 : r - R0 + 8, :] - SCALE * out
                rp[x, r : r + 8, :] = out
                acc = acc + out * out
            return acc

        return over(planes, body, acc, max(2, 16 // len(chunks) // 2 * 2))

    def power(f, w, planes, chunks, acc):
        def body(x, acc):
            cross, square = acc
            for r in chunks:
                centre, out = apply(f, x, r)
                if w is not None:
                    w[x, r : r + 8, :] = out
                cross, square = cross + centre * out, square + out * out
            return cross, square

        return over(planes, body, acc, max(2, 16 // len(chunks) // 2 * 2))

    def body(x, c):
        weights_x(x, whole)
        for r in whole[:-1]:
            weights_y(x, r)
        weights_y(x, R1 - 8, 4)
        for r in whole:
            weights_z(x, r)
        for r in inner:
            add_diagonal(x, r)
        return c

    with jax.named_scope("weights"):
        weights_x(1, whole)
        lax.fori_loop(2, 32, body, 0)
        for x in (1, 32):
            for r in whole[:-1]:
                weights_y(x, r)
            weights_y(x, R1 - 8, 4)
            for r in whole:
                weights_z(x, r)
    with jax.named_scope("r_inner"):
        for copy in loads[8:]:
            copy.wait()
        zero = jnp.zeros((8, 128), F32)
        m0 = residual(range(2, 32), inner, zero)
    with jax.named_scope("wait_k_x"):
        arrived(0, kp, ("gx",))
    weights_x(0, whole)
    weights_x(32, whole)
    for x in (1, 32):
        for r in inner:
            add_diagonal(x, r)
    arrived(1, up, ("gx",))
    m0 = residual((1, 32), inner, m0)
    with jax.named_scope("wait_k_y"):
        arrived(0, kp, ("gy",))

    def body(x, c):
        weights_y(x, R0 - 4, 4)
        weights_y(x, R1 - 4, 4)
        for r in ends:
            add_diagonal(x, r)
        return c

    over(range(1, 33), body, 0, 4)
    with jax.named_scope("wait_u_y_r_ring"):
        arrived(1, up, ("gy",))
        m0 = residual(range(1, 33), ends, m0)

    moments = [m0]
    for e, (f, w) in enumerate(((rp, v1), (v1, v2), (v2, None)), start=2):
        exchange(e, f)
        with jax.named_scope("inner%d" % e):
            acc = power(f, w, range(2, 32), inner, (zero, zero))
        with jax.named_scope("waitx%d" % e):
            arrived(e, f, ("gx",))
        with jax.named_scope("ringx%d" % e):
            acc = power(f, w, (1, 32), inner, acc)
        with jax.named_scope("waity%d" % e):
            arrived(e, f, ("gy",))
        with jax.named_scope("ringy%d" % e):
            acc = power(f, w, range(1, 33), ends, acc)
        moments.extend(acc)

    with jax.named_scope("moments"):
        sub = lax.broadcasted_iota(jnp.int32, (8, 128), 0)
        stacked = zero
        for k, m in enumerate(moments):
            stacked = jnp.where(sub == k, jnp.sum(m, axis=0, keepdims=True), stacked)
        sums = jnp.sum(stacked, axis=1, keepdims=True)
        own = jnp.sum(jnp.where(lane == sub, sums, 0.0), axis=0, keepdims=True)
        place = gx * ngy + gy
    row[...] = own
    gath[pl.ds(place, 1), :] = own
    pl.semaphore_wait(ready, ngx - 1)

    with jax.named_scope("gsend"):
        for dx, dy in far_first(ngx, ngy):
            pltpu.make_async_remote_copy(
                src_ref=row, dst_ref=gath.at[pl.ds(place, 1), :], send_sem=gsend, recv_sem=grecv,
                device_id=(lax.rem(gx + dx, ngx), lax.rem(gy + dy, ngy)), device_id_type=MESH,
            ).start()
    every = pltpu.make_async_remote_copy(
        src_ref=gath.at[0 : count - 1, :], dst_ref=gath.at[0 : count - 1, :], send_sem=gsend, recv_sem=grecv,
        device_id=(gx, gy), device_id_type=MESH,
    )
    with jax.named_scope("gwait"):
        every.wait_recv()
    with jax.named_scope("solve"):
        table = gath[...]
        bound = 2.0 * jnp.sum(jnp.abs(table), axis=0, keepdims=True)
        upper = (table + bound) - bound
        high = jnp.sum(upper, axis=0, keepdims=True)
        low = jnp.sum(table - upper, axis=0, keepdims=True)
        lane1 = lax.broadcasted_iota(jnp.int32, (1, 128), 1)

        def pick(v, k):
            return jnp.sum(jnp.where(lane1 == k, v, 0.0), axis=1, keepdims=True)

        m = [renorm(pick(high, k), pick(low, k)) for k in range(7)]
        (y1, y2, y3), rest = normal_equations(m)
        est_ref[...] = jnp.broadcast_to(jnp.sqrt(jnp.maximum(rest, 0.0)), (1, 128))
        y1, y2, y3 = (jnp.broadcast_to(y, (8, 128)) for y in (y1, y2, y3))

    def body(x, c):
        for r in whole:
            s = slice(r, r + 8)
            sol_ref[x - 1, r - R0 : r - R0 + 8, :] = up[x, s, :] + (
                y1 * rp[x, s, :] + (y2 * v1[x, s, :] + y3 * v2[x, s, :])
            )
        return c

    with jax.named_scope("final"):
        lax.fori_loop(1, 33, body, 0)
    every.wait_send()
    for e, f in enumerate((kp, up, rp, v1, v2)):
        sent(e, f)


def local(ngx, ngy, right_side, start_guess, conductivity):
    field = pltpu.VMEM((PLANES, ROWS, 128), F32)
    block = pltpu.VMEM((32, 128, 128), F32)
    sem = pltpu.SemaphoreType
    sol, est = pl.pallas_call(
        functools.partial(kernel, ngx, ngy),
        out_shape=(jax.ShapeDtypeStruct((32, 128, 128), F32), jax.ShapeDtypeStruct((1, 128), F32)),
        in_specs=[pl.BlockSpec(memory_space=pltpu.HBM)] * 3,
        out_specs=(pl.BlockSpec(memory_space=pltpu.VMEM), pl.BlockSpec(memory_space=pltpu.VMEM)),
        scratch_shapes=[field] * 5 + [
            block,
            pltpu.VMEM((33, 128, 128), F32),
            pltpu.VMEM((33, ROWS, 128), F32),
            pltpu.VMEM((33, 128, 128), F32),
            pltpu.VMEM((33, 128, 128), F32),
            pltpu.VMEM((33, 128, 128), F32),
            pltpu.VMEM((1, 128), F32),
            pltpu.VMEM((ngx * ngy, 128), F32),
            sem.DMA((3, 4)), sem.DMA((5, 4)), sem.DMA((5, 4)), sem.DMA, sem.DMA, sem.REGULAR,
        ],
        compiler_params=pltpu.CompilerParams(
            collective_id=0, has_side_effects=True, vmem_limit_bytes=int(50 * 2**20)
        ),
    )(right_side, start_guess, conductivity)
    return sol.reshape(32, 32, 512), est[0, 0]


def solution(mesh):
    return jax.shard_map(
        functools.partial(local, mesh.shape["gx"], mesh.shape["gy"]),
        mesh=mesh,
        in_specs=(P("gx", "gy", None),) * 3,
        out_specs=(P("gx", "gy", None), P()),
        check_vma=False,
    )
```

```python
import functools

import jax
import jax.numpy as jnp
from jax import lax
from jax.experimental import pallas as pl
from jax.experimental.pallas import tpu as pltpu
from jax.sharding import PartitionSpec as P

MESH = pl.DeviceIdType.MESH
F32 = jnp.float32
SCALE = 64.0
HALF = 0.5 / SCALE
X0, X1 = 2, 34
R0, R1 = 16, 144
PLANES, ROWS = 36, 160


def renorm(a, b):
    s = a + b
    return s, b - (s - a)


def two_sum(a, b):
    s = a + b
    t = s - a
    return s, (a - (s - t)) + (b - t)


def split(a):
    t = 4097.0 * a
    high = t - (t - a)
    return high, a - high


def two_prod(a, b):
    p = a * b
    (ah, al), (bh, bl) = split(a), split(b)
    return p, ((ah * bh - p) + ah * bl + al * bh) + al * bl


def add(a, b):
    s, e = two_sum(a[0], b[0])
    return renorm(s, e + (a[1] + b[1]))


def sub(a, b):
    return add(a, (-b[0], -b[1]))


def mul(a, b):
    p, e = two_prod(a[0], b[0])
    return renorm(p, e + (a[0] * b[1] + a[1] * b[0]))


def div(a, b):
    q = a[0] / b[0]
    p, e = two_prod(q, b[0])
    return renorm(q, (((a[0] - p) - e) + (a[1] - q * b[1])) / b[0])


def split_sum(v, axis):
    bound = 2.0 * jnp.sum(jnp.abs(v), axis=axis, keepdims=True)
    upper = (v + bound) - bound
    return jnp.sum(upper, axis=axis, keepdims=True), jnp.sum(v - upper, axis=axis, keepdims=True)


def normal_equations(m):
    l21, l31 = div(m[3], m[2]), div(m[4], m[2])
    d2 = sub(m[4], mul(l21, m[3]))
    e2 = sub(m[5], mul(l21, m[4]))
    l32 = div(e2, d2)
    d3 = sub(sub(m[6], mul(l31, m[4])), mul(l32, e2))
    c1 = m[1]
    c2 = sub(m[2], mul(l21, c1))
    c3 = sub(sub(m[3], mul(l31, c1)), mul(l32, c2))
    q1, q2, q3 = div(c1, m[2]), div(c2, d2), div(c3, d3)
    y3 = q3
    y2 = sub(q2, mul(l32, y3))
    y1 = sub(sub(q1, mul(l21, y2)), mul(l31, y3))
    rest = sub(sub(sub(m[0], mul(c1, q1)), mul(c2, q2)), mul(c3, q3))
    return tuple(y[0] / SCALE for y in (y1, y2, y3)), rest[0]


def directions(gx, gy, ngx, ngy):
    out = []
    for sx, sy in ((0, 1), (0, -1), (1, 0), (-1, 0), (1, 1), (1, -1), (-1, 1), (-1, -1)):
        to, come = [], []
        for step, at, n in ((sx, gx, ngx), (sy, gy, ngy)):
            if step:
                to.append(at < n - 1 if step > 0 else at > 0)
                come.append(at > 0 if step > 0 else at < n - 1)
        both = (lambda c: c[0]) if len(to) == 1 else (lambda c: jnp.logical_and(*c))
        out.append((sx, sy, both(to), both(come)))
    return out


def far_first(ngx, ngy):
    def ring(d):
        return min(d % 4, -d % 4)

    offsets = [(dx, dy) for dx in range(ngx) for dy in range(ngy) if dx or dy]
    return sorted(offsets, key=lambda o: -(ring(o[0] // 2) + ring(o[1] // 4) + ring(o[1] % 4)))


def extent(step, low, high, depth, outside):
    if step == 0:
        return slice(low, high)
    if outside:
        return slice(low - depth, low) if step > 0 else slice(high, high + depth)
    return slice(high - depth, high) if step > 0 else slice(low, low + depth)


def piece(ref, sx, sy, depth, outside):
    if sx and sy:
        depth = 1
    return ref.at[extent(sx, X0, X1, depth, outside), extent(sy, R0, R1, 4 * depth, outside), :]


def kernel(
    ngx, ngy,
    rhs_hbm, x0_hbm, k_hbm, sol_ref, est_ref,
    kp, up, rb, rp, v1, v2, wx, wy, wzm, wzp, dg, row, gath,
    load_sem, send_sem, recv_sem, gsend, grecv, ready,
):
    gx, gy = lax.axis_index("gx"), lax.axis_index("gy")
    count = ngx * ngy
    loads = []
    for i, (src, dst) in enumerate(((k_hbm, kp), (x0_hbm, up), (rhs_hbm, rb))):
        view = dst.reshape(PLANES, ROWS // 4, 4, 128)
        for q in range(4):
            loads.append(
                pltpu.make_async_copy(
                    src.at[:, :, q * 128 : (q + 1) * 128],
                    view.at[X0:X1, R0 // 4 : R1 // 4, q, :],
                    load_sem.at[i, q],
                )
            )
    for copy in loads:
        copy.start()

    barrier = pltpu.get_barrier_semaphore()
    greet = [(d, 0) for d in range(1, ngx)] + [(0, d) for d in range(1, ngy)]
    greet += [(1, 1), (1, ngy - 1), (ngx - 1, 1), (ngx - 1, ngy - 1)]
    for dx, dy in greet:
        pl.semaphore_signal(
            barrier, inc=1, device_id=(lax.rem(gx + dx, ngx), lax.rem(gy + dy, ngy)), device_id_type=MESH
        )

    dirs = directions(gx, gy, ngx, ngy)
    has_low_x, has_high_x, has_low_y, has_high_y = gx > 0, gx < ngx - 1, gy > 0, gy < ngy - 1
    fields = (kp, up, rp, v1, v2)
    zero = jnp.zeros((8, 128), F32)

    for at, inside in ((0, has_low_x), (X1, has_high_x)):

        @pl.when(jnp.logical_not(inside))
        def _():
            def fill(i, c):
                for f in fields:
                    for x in (at, at + 1):
                        f[x, pl.ds(pl.multiple_of(8 + 8 * i, 8), 8), :] = zero
                return c

            lax.fori_loop(0, 18, fill, 0)

    for at, inside in ((R0 - 8, has_low_y), (R1, has_high_y)):

        @pl.when(jnp.logical_not(inside))
        def _():
            def fill(x, c):
                for f in fields:
                    f[x, at : at + 8, :] = zero
                return c

            lax.fori_loop(0, PLANES, fill, 0)

    def copy_of(e, f, depth, i):
        sx, sy = dirs[i][:2]
        return pltpu.make_async_remote_copy(
            src_ref=piece(f, sx, sy, depth, False), dst_ref=piece(f, sx, sy, depth, True),
            send_sem=send_sem.at[e, i], recv_sem=recv_sem.at[e, i],
            device_id={"gx": lax.rem(gx + sx + ngx, ngx), "gy": lax.rem(gy + sy + ngy, ngy)},
            device_id_type=MESH,
        )

    def exchange(e, f, depth, which):
        for i in which:

            @pl.when(dirs[i][2])
            def _():
                copy_of(e, f, depth, i).start()

    def arrived(e, f, depth, which):
        for i in which:

            @pl.when(dirs[i][3])
            def _():
                copy_of(e, f, depth, i).wait_recv()

    def sent(e, f, depth, which):
        for i in which:

            @pl.when(dirs[i][2])
            def _():
                copy_of(e, f, depth, i).wait_send()

    along_y, along_x, corners = (0, 1), (2, 3), (4, 5, 6, 7)
    every_way = along_y + along_x + corners
    faces = along_y + along_x

    with jax.named_scope("load_k"):
        for copy in loads[:4]:
            copy.wait()
    with jax.named_scope("barrier"):
        pl.semaphore_wait(barrier, len(greet))
        exchange(0, kp, 2, every_way)
        for copy in loads[4:8]:
            copy.wait()
        exchange(1, up, 2, every_way)
        for copy in loads[8:]:
            copy.wait()
        exchange(2, rb, 1, faces)
        for d in range(1, ngx):
            pl.semaphore_signal(ready, inc=1, device_id=(lax.rem(gx + d, ngx), gy), device_id_type=MESH)

    lane = lax.broadcasted_iota(jnp.int32, (8, 128), 1)
    sub = lax.broadcasted_iota(jnp.int32, (8, 128), 0)
    zhi = lax.rem(sub, 4)
    first_lane, last_lane = lane == 0, lane == 127
    z_first = jnp.logical_and(first_lane, zhi == 0)
    z_last = jnp.logical_and(last_lane, zhi == 3)

    def z_up(f, x, r, centre):
        return pltpu.roll(jnp.where(first_lane, f[x, r + 1 : r + 9, :], centre), 127, 1)

    def z_down(f, x, r, centre):
        return pltpu.roll(jnp.where(last_lane, f[x, r - 1 : r + 7, :], centre), 1, 1)

    def weights_x(i, r):
        wx[i, r : r + 8, :] = HALF * (kp[i, r : r + 8, :] + kp[i + 1, r : r + 8, :])

    def weights_y(x, r, n=8):
        wy[x, r : r + n, :] = HALF * (kp[x, r : r + n, :] + kp[x, r + 4 : r + 4 + n, :])

    def weights_z(x, r):
        centre = kp[x, r : r + 8, :]
        above = jnp.where(first_lane, pltpu.roll(centre, 7, 0), centre)
        below = jnp.where(last_lane, pltpu.roll(centre, 1, 0), centre)
        up_w = HALF * (centre + jnp.where(z_last, 0.0, pltpu.roll(above, 127, 1)))
        down_w = HALF * (centre + jnp.where(z_first, 0.0, pltpu.roll(below, 1, 1)))
        dg[x, r : r + 8, :] = up_w + down_w
        wzp[x, r : r + 8, :] = jnp.where(z_last, 0.0, up_w)
        wzm[x, r : r + 8, :] = jnp.where(z_first, 0.0, down_w)

    def add_diagonal(x, r):
        s = slice(r, r + 8)
        dg[x, s, :] = dg[x, s, :] + ((wx[x - 1, s, :] + wx[x, s, :]) + (wy[x, r - 4 : r + 4, :] + wy[x, s, :]))

    def apply(f, x, r):
        s = slice(r, r + 8)
        centre = f[x, s, :]
        out = dg[x, s, :] * centre
        out = out - wx[x - 1, s, :] * f[x - 1, s, :]
        out = out - wx[x, s, :] * f[x + 1, s, :]
        out = out - wy[x, r - 4 : r + 4, :] * f[x, r - 4 : r + 4, :]
        out = out - wy[x, s, :] * f[x, r + 4 : r + 12, :]
        out = out - wzm[x, s, :] * z_down(f, x, r, centre)
        out = out - wzp[x, s, :] * z_up(f, x, r, centre)
        return centre, out

    def chunks(first, last):
        return tuple(range(R0 + 4 * first, R0 + 4 * last, 8))

    def over(planes, body, carry, unroll=1):
        if not isinstance(planes, range):
            for x in planes:
                carry = body(x, carry)
            return carry
        first, steps = planes.start, len(planes) // unroll

        def several(i, carry):
            for u in range(unroll):
                carry = body(first + i * unroll + u, carry)
            return carry

        return lax.fori_loop(0, steps, several, carry)

    def step(f, w, counted):
        def run(planes, rows, acc, unroll=1):
            def body(x, acc):
                own = (zero,) * counted
                for r in rows:
                    centre, out = apply(f, x, r)
                    if f is up:
                        out = rb[x, r : r + 8, :] - SCALE * out
                    if w is not None:
                        w[x, r : r + 8, :] = out
                    if acc is not None and counted == 1:
                        own = (own[0] + out * out,)
                    elif acc is not None:
                        own = (own[0] + centre * out, own[1] + out * out)
                return None if acc is None else tuple(a + o for a, o in zip(acc, own))

            if acc is None:
                over(planes, lambda x, c: (body(x, None), c)[1], 0, unroll)
                return None
            return over(planes, body, acc, unroll)

        return run

    def when(flag, fn):
        pl.when(flag)(fn)

    def two_steps(name, first, second, acc1, acc2, wait_x, wait_y, between):
        with jax.named_scope(name + "_in1"):
            acc1 = first(range(X0 + 1, X1 - 1), chunks(2, 29), acc1, 2)
        with jax.named_scope(name + "_in2"):
            acc2 = second(range(X0 + 2, X1 - 2), chunks(4, 27), acc2, 2)
        between()
        with jax.named_scope(name + "_waitx"):
            wait_x()
        with jax.named_scope(name + "_ringx"):
            acc1 = first((X0, X1 - 1), chunks(2, 29), acc1)
            when(has_low_x, lambda: first((X0 - 1,), chunks(2, 29), None))
            when(has_high_x, lambda: first((X1,), chunks(2, 29), None))
            acc2 = second((X0, X0 + 1, X1 - 2, X1 - 1), chunks(4, 27), acc2)
        with jax.named_scope(name + "_waity"):
            wait_y()
        with jax.named_scope(name + "_ringy1"):
            acc1 = first(range(X0, X1), chunks(0, 1) + chunks(30, 31), acc1, 4)
            when(has_low_x, lambda: first((X0 - 1,), chunks(0, 1) + chunks(30, 31), None))
            when(has_high_x, lambda: first((X1,), chunks(0, 1) + chunks(30, 31), None))
            when(has_low_y, lambda: first(range(X0, X1), chunks(-2, -1), None, 8))
            when(has_high_y, lambda: first(range(X0, X1), chunks(32, 33), None, 8))
        with jax.named_scope(name + "_ringy2"):
            acc2 = second(range(X0, X1), chunks(0, 3) + chunks(28, 31), acc2, 4)
        return acc1, acc2

    own = chunks(0, 31)
    inner = chunks(2, 29)
    ends = chunks(0, 1) + chunks(30, 31)

    def own_weights(x, c, with_x=True, diagonal=True):
        for r in own:
            if with_x:
                weights_x(x, r)
            weights_z(x, r)
        for r in own[:-1]:
            weights_y(x, r)
        weights_y(x, R1 - 8, 4)
        if diagonal:
            for r in inner:
                add_diagonal(x, r)
        return c

    with jax.named_scope("weights"):
        own_weights(X0, 0, diagonal=False)
        over(range(X0 + 1, X1 - 1), own_weights, 0, 2)
        own_weights(X1 - 1, 0, with_x=False, diagonal=False)

    def halo_weights():
        with jax.named_scope("wait_k"):
            arrived(0, kp, 2, every_way)
        with jax.named_scope("halo_weights"):
            for i in (X0 - 2, X0 - 1, X1 - 1, X1):
                for r in own:
                    weights_x(i, r)
            for x in (X0 - 1, X1):
                for r in own:
                    weights_z(x, r)
                    weights_y(x, r)
                weights_y(x, R0 - 4, 4)
                for r in own:
                    add_diagonal(x, r)
            for r in (R0 - 8, R1):
                weights_x(X0 - 1, r)

            def body(x, c):
                weights_y(x, R0 - 8, 8)
                weights_y(x, R1 - 4, 8)
                for r in (R0 - 8, R1):
                    weights_x(x, r)
                    weights_z(x, r)
                for r in (R0 - 8, R1) + ends:
                    add_diagonal(x, r)
                return c

            over(range(X0, X1), body, 0, 4)
            for x in (X0, X1 - 1):
                for r in inner:
                    add_diagonal(x, r)

    def wait_fields_x():
        arrived(1, up, 2, along_x)
        arrived(2, rb, 1, along_x)

    def wait_fields_y():
        arrived(1, up, 2, along_y + corners)
        arrived(2, rb, 1, along_y)

    pair = (zero, zero)
    (m0,), (m1, m2) = two_steps(
        "p1", step(up, rp, 1), step(rp, v1, 2), (zero,), pair, wait_fields_x, wait_fields_y, halo_weights
    )
    exchange(3, v1, 2, every_way)
    (m3, m4), (m5, m6) = two_steps(
        "p2", step(v1, v2, 2), step(v2, None, 2), pair, pair,
        lambda: arrived(3, v1, 2, along_x), lambda: arrived(3, v1, 2, along_y + corners), lambda: None,
    )
    moments = [m0, m1, m2, m3, m4, m5, m6]

    with jax.named_scope("moments"):
        stacked = zero
        for k, m in enumerate(moments):
            stacked = jnp.where(sub == k, jnp.sum(m, axis=0, keepdims=True), stacked)
        high, low = split_sum(stacked, 1)
        mine = jnp.sum(jnp.where(lane == sub, high, jnp.where(lane == sub + 8, low, 0.0)), axis=0, keepdims=True)
    place = gx * ngy + gy
    row[...] = mine
    gath[pl.ds(place, 1), :] = mine
    pl.semaphore_wait(ready, ngx - 1)
    with jax.named_scope("gsend"):
        for dx, dy in far_first(ngx, ngy):
            pltpu.make_async_remote_copy(
                src_ref=row, dst_ref=gath.at[pl.ds(place, 1), :], send_sem=gsend, recv_sem=grecv,
                device_id=(lax.rem(gx + dx, ngx), lax.rem(gy + dy, ngy)), device_id_type=MESH,
            ).start()
    every = pltpu.make_async_remote_copy(
        src_ref=gath.at[0 : count - 1, :], dst_ref=gath.at[0 : count - 1, :], send_sem=gsend, recv_sem=grecv,
        device_id=(gx, gy), device_id_type=MESH,
    )
    with jax.named_scope("gwait"):
        every.wait_recv()
    with jax.named_scope("solve"):
        high, low = split_sum(gath[...], 0)
        lane1 = lax.broadcasted_iota(jnp.int32, (1, 128), 1)

        def pick(v, k):
            return jnp.sum(jnp.where(lane1 == k, v, 0.0), axis=1, keepdims=True)

        m = [renorm(pick(high, k), pick(low, k) + pick(high + low, k + 8)) for k in range(7)]
        (y1, y2, y3), rest = normal_equations(m)
        est_ref[...] = jnp.broadcast_to(jnp.sqrt(jnp.maximum(rest, 0.0)), (1, 128))
        y1, y2, y3 = (jnp.broadcast_to(y, (8, 128)) for y in (y1, y2, y3))

    def combine(x, c):
        for r in own:
            s = slice(r, r + 8)
            sol_ref[x - X0, r - R0 : r - R0 + 8, :] = up[x, s, :] + (
                y1 * rp[x, s, :] + (y2 * v1[x, s, :] + y3 * v2[x, s, :])
            )
        return c

    with jax.named_scope("final"):
        over(range(X0, X1), combine, 0, 2)
    every.wait_send()
    sent(0, kp, 2, every_way)
    sent(1, up, 2, every_way)
    sent(2, rb, 1, faces)
    sent(3, v1, 2, every_way)


def local(ngx, ngy, right_side, start_guess, conductivity):
    field = pltpu.VMEM((PLANES, ROWS, 128), F32)
    sem = pltpu.SemaphoreType
    sol, est = pl.pallas_call(
        functools.partial(kernel, ngx, ngy),
        out_shape=(jax.ShapeDtypeStruct((32, 128, 128), F32), jax.ShapeDtypeStruct((1, 128), F32)),
        in_specs=[pl.BlockSpec(memory_space=pltpu.HBM)] * 3,
        out_specs=(pl.BlockSpec(memory_space=pltpu.VMEM), pl.BlockSpec(memory_space=pltpu.VMEM)),
        scratch_shapes=[field] * 11 + [
            pltpu.VMEM((1, 128), F32),
            pltpu.VMEM((ngx * ngy, 128), F32),
            sem.DMA((3, 4)), sem.DMA((4, 8)), sem.DMA((4, 8)), sem.DMA, sem.DMA, sem.REGULAR,
        ],
        compiler_params=pltpu.CompilerParams(
            collective_id=0, has_side_effects=True, vmem_limit_bytes=50 * 2**20
        ),
    )(right_side, start_guess, conductivity)
    return sol.reshape(32, 32, 512), est[0, 0]


def solution(mesh):
    return jax.shard_map(
        functools.partial(local, mesh.shape["gx"], mesh.shape["gy"]),
        mesh=mesh,
        in_specs=(P("gx", "gy", None),) * 3,
        out_specs=(P("gx", "gy", None), P()),
        check_vma=False,
    )
```

```python
import functools

import jax
import jax.numpy as jnp
from jax import lax
from jax.experimental import pallas as pl
from jax.experimental.pallas import tpu as pltpu
from jax.sharding import PartitionSpec as P

MESH = pl.DeviceIdType.MESH
F32 = jnp.float32
SCALE = 64.0
HALF = 0.5 / SCALE
X0, X1 = 2, 34
R0, R1 = 16, 144
PLANES, ROWS = 36, 160
UW, U1, U2, UY = 5, 5, 4, 8


def renorm(a, b):
    s = a + b
    return s, b - (s - a)


def two_sum(a, b):
    s = a + b
    t = s - a
    return s, (a - (s - t)) + (b - t)


def split(a):
    t = 4097.0 * a
    high = t - (t - a)
    return high, a - high


def two_prod(a, b):
    p = a * b
    (ah, al), (bh, bl) = split(a), split(b)
    return p, ((ah * bh - p) + ah * bl + al * bh) + al * bl


def add(a, b):
    s, e = two_sum(a[0], b[0])
    return renorm(s, e + (a[1] + b[1]))


def sub(a, b):
    return add(a, (-b[0], -b[1]))


def mul(a, b):
    p, e = two_prod(a[0], b[0])
    return renorm(p, e + (a[0] * b[1] + a[1] * b[0]))


def div(a, b):
    q = a[0] / b[0]
    p, e = two_prod(q, b[0])
    return renorm(q, (((a[0] - p) - e) + (a[1] - q * b[1])) / b[0])


def split_sum(v, axis):
    bound = 2.0 * jnp.sum(jnp.abs(v), axis=axis, keepdims=True)
    upper = (v + bound) - bound
    return jnp.sum(upper, axis=axis, keepdims=True), jnp.sum(v - upper, axis=axis, keepdims=True)


def normal_equations(m):
    l21, l31 = div(m[3], m[2]), div(m[4], m[2])
    d2 = sub(m[4], mul(l21, m[3]))
    e2 = sub(m[5], mul(l21, m[4]))
    l32 = div(e2, d2)
    d3 = sub(sub(m[6], mul(l31, m[4])), mul(l32, e2))
    c1 = m[1]
    c2 = sub(m[2], mul(l21, c1))
    c3 = sub(sub(m[3], mul(l31, c1)), mul(l32, c2))
    q1, q2, q3 = div(c1, m[2]), div(c2, d2), div(c3, d3)
    y3 = q3
    y2 = sub(q2, mul(l32, y3))
    y1 = sub(sub(q1, mul(l21, y2)), mul(l31, y3))
    rest = sub(sub(sub(m[0], mul(c1, q1)), mul(c2, q2)), mul(c3, q3))
    return tuple(y[0] / SCALE for y in (y1, y2, y3)), rest[0]


def directions(gx, gy, ngx, ngy):
    out = []
    for sx, sy in ((0, 1), (0, -1), (1, 0), (-1, 0), (1, 1), (1, -1), (-1, 1), (-1, -1)):
        to, come = [], []
        for step, at, n in ((sx, gx, ngx), (sy, gy, ngy)):
            if step:
                to.append(at < n - 1 if step > 0 else at > 0)
                come.append(at > 0 if step > 0 else at < n - 1)
        both = (lambda c: c[0]) if len(to) == 1 else (lambda c: jnp.logical_and(*c))
        out.append((sx, sy, both(to), both(come)))
    return out


def far_first(ngx, ngy):
    def ring(d):
        return min(d % 4, -d % 4)

    offsets = [(dx, dy) for dx in range(ngx) for dy in range(ngy) if dx or dy]
    return sorted(offsets, key=lambda o: -(ring(o[0] // 2) + ring(o[1] // 4) + ring(o[1] % 4)))


def extent(step, low, high, depth, outside):
    if step == 0:
        return slice(low, high)
    if outside:
        return slice(low - depth, low) if step > 0 else slice(high, high + depth)
    return slice(high - depth, high) if step > 0 else slice(low, low + depth)


def piece(ref, sx, sy, depth, outside):
    if sx and sy:
        depth = 1
    return ref.at[extent(sx, X0, X1, depth, outside), extent(sy, R0, R1, 4 * depth, outside), :]


def kernel(
    ngx, ngy,
    rhs_hbm, x0_hbm, k_hbm, sol_ref, est_ref,
    kp, up, rb, rp, v1, v2, wx, wy, wzm, wzp, dg, row, gath,
    load_sem, send_sem, recv_sem, gsend, grecv, ready,
):
    gx, gy = lax.axis_index("gx"), lax.axis_index("gy")
    count = ngx * ngy
    loads = []
    for i, (src, dst) in enumerate(((k_hbm, kp), (x0_hbm, up), (rhs_hbm, rb))):
        view = dst.reshape(PLANES, ROWS // 4, 4, 128)
        for q in range(4):
            loads.append(
                pltpu.make_async_copy(
                    src.at[:, :, q * 128 : (q + 1) * 128],
                    view.at[X0:X1, R0 // 4 : R1 // 4, q, :],
                    load_sem.at[i, q],
                )
            )
    for copy in loads:
        copy.start()

    barrier = pltpu.get_barrier_semaphore()
    greet = [(d, 0) for d in range(1, ngx)] + [(0, d) for d in range(1, ngy)]
    greet += [(1, 1), (1, ngy - 1), (ngx - 1, 1), (ngx - 1, ngy - 1)]
    for dx, dy in greet:
        pl.semaphore_signal(
            barrier, inc=1, device_id=(lax.rem(gx + dx, ngx), lax.rem(gy + dy, ngy)), device_id_type=MESH
        )

    dirs = directions(gx, gy, ngx, ngy)
    has_low_x, has_high_x, has_low_y, has_high_y = gx > 0, gx < ngx - 1, gy > 0, gy < ngy - 1
    fields = (kp, up, rp, v1, v2)
    zero = jnp.zeros((8, 128), F32)

    for at, inside in ((0, has_low_x), (X1, has_high_x)):

        @pl.when(jnp.logical_not(inside))
        def _():
            def fill(i, c):
                for f in fields:
                    for x in (at, at + 1):
                        f[x, pl.ds(pl.multiple_of(8 + 8 * i, 8), 8), :] = zero
                return c

            lax.fori_loop(0, 18, fill, 0)

    for at, inside in ((R0 - 8, has_low_y), (R1, has_high_y)):

        @pl.when(jnp.logical_not(inside))
        def _():
            def fill(x, c):
                for f in fields:
                    f[x, at : at + 8, :] = zero
                return c

            lax.fori_loop(0, PLANES, fill, 0)

    def copy_of(e, f, depth, i):
        sx, sy = dirs[i][:2]
        return pltpu.make_async_remote_copy(
            src_ref=piece(f, sx, sy, depth, False), dst_ref=piece(f, sx, sy, depth, True),
            send_sem=send_sem.at[e, i], recv_sem=recv_sem.at[e, i],
            device_id={"gx": lax.rem(gx + sx + ngx, ngx), "gy": lax.rem(gy + sy + ngy, ngy)},
            device_id_type=MESH,
        )

    def exchange(e, f, depth, which):
        for i in which:

            @pl.when(dirs[i][2])
            def _():
                copy_of(e, f, depth, i).start()

    def arrived(e, f, depth, which):
        for i in which:

            @pl.when(dirs[i][3])
            def _():
                copy_of(e, f, depth, i).wait_recv()

    def sent(e, f, depth, which):
        for i in which:

            @pl.when(dirs[i][2])
            def _():
                copy_of(e, f, depth, i).wait_send()

    along_y, along_x, corners = (0, 1), (2, 3), (4, 5, 6, 7)
    every_way = along_y + along_x + corners
    faces = along_y + along_x

    with jax.named_scope("load_k"):
        for copy in loads[:4]:
            copy.wait()
    with jax.named_scope("barrier"):
        pl.semaphore_wait(barrier, len(greet))
        exchange(0, kp, 2, every_way)
        for d in range(1, ngx):
            pl.semaphore_signal(ready, inc=1, device_id=(lax.rem(gx + d, ngx), gy), device_id_type=MESH)

    lane = lax.broadcasted_iota(jnp.int32, (8, 128), 1)
    sub = lax.broadcasted_iota(jnp.int32, (8, 128), 0)
    zhi = lax.rem(sub, 4)
    first_lane, last_lane = lane == 0, lane == 127
    z_first = jnp.logical_and(first_lane, zhi == 0)
    z_last = jnp.logical_and(last_lane, zhi == 3)

    def z_up(f, x, r, centre):
        return pltpu.roll(jnp.where(first_lane, f[x, r + 1 : r + 9, :], centre), 127, 1)

    def z_down(f, x, r, centre):
        return pltpu.roll(jnp.where(last_lane, f[x, r - 1 : r + 7, :], centre), 1, 1)

    def weights_x(i, r):
        wx[i, r : r + 8, :] = HALF * (kp[i, r : r + 8, :] + kp[i + 1, r : r + 8, :])

    def weights_y(x, r, n=8):
        wy[x, r : r + n, :] = HALF * (kp[x, r : r + n, :] + kp[x, r + 4 : r + 4 + n, :])

    def weights_z(x, r):
        centre = kp[x, r : r + 8, :]
        above = jnp.where(first_lane, pltpu.roll(centre, 7, 0), centre)
        below = jnp.where(last_lane, pltpu.roll(centre, 1, 0), centre)
        up_w = HALF * (centre + jnp.where(z_last, 0.0, pltpu.roll(above, 127, 1)))
        down_w = HALF * (centre + jnp.where(z_first, 0.0, pltpu.roll(below, 1, 1)))
        dg[x, r : r + 8, :] = up_w + down_w
        wzp[x, r : r + 8, :] = jnp.where(z_last, 0.0, up_w)
        wzm[x, r : r + 8, :] = jnp.where(z_first, 0.0, down_w)

    def add_diagonal(x, r):
        s = slice(r, r + 8)
        dg[x, s, :] = dg[x, s, :] + ((wx[x - 1, s, :] + wx[x, s, :]) + (wy[x, r - 4 : r + 4, :] + wy[x, s, :]))

    def apply(f, x, r):
        s = slice(r, r + 8)
        centre = f[x, s, :]
        out = dg[x, s, :] * centre
        out = out - wx[x - 1, s, :] * f[x - 1, s, :]
        out = out - wx[x, s, :] * f[x + 1, s, :]
        out = out - wy[x, r - 4 : r + 4, :] * f[x, r - 4 : r + 4, :]
        out = out - wy[x, s, :] * f[x, r + 4 : r + 12, :]
        out = out - wzm[x, s, :] * z_down(f, x, r, centre)
        out = out - wzp[x, s, :] * z_up(f, x, r, centre)
        return centre, out

    def chunks(first, last):
        return tuple(range(R0 + 4 * first, R0 + 4 * last, 8))

    def over(planes, body, carry, unroll=1):
        if not isinstance(planes, range):
            for x in planes:
                carry = body(x, carry)
            return carry
        first, steps = planes.start, len(planes) // unroll

        def several(i, carry):
            for u in range(unroll):
                carry = body(first + i * unroll + u, carry)
            return carry

        return lax.fori_loop(0, steps, several, carry)

    def step(f, w, counted):
        def run(planes, rows, acc, unroll=1):
            def body(x, acc):
                own = (zero,) * counted
                for r in rows:
                    centre, out = apply(f, x, r)
                    if f is up:
                        out = rb[x, r : r + 8, :] - SCALE * out
                    inside = True
                    for at, low, high, below, beyond in (
                        (x, X0, X1, has_low_x, has_high_x), (r, R0, R1, has_low_y, has_high_y)
                    ):
                        if isinstance(at, int) and not low <= at < high:
                            inside = False
                            out = jnp.where(below if at < low else beyond, out, 0.0)
                    if w is not None:
                        w[x, r : r + 8, :] = out
                    if inside and counted == 1:
                        own = (own[0] + out * out,)
                    elif inside:
                        own = (own[0] + centre * out, own[1] + out * out)
                return tuple(a + o for a, o in zip(acc, own))

            return over(planes, body, acc, unroll)

        return run

    def two_steps(name, first, second, acc1, acc2, wait_x, wait_y, between):
        with jax.named_scope(name + "_in1"):
            acc1 = first(range(X0 + 1, X1 - 1), chunks(2, 29), acc1, U1)
        with jax.named_scope(name + "_in2"):
            acc2 = second(range(X0 + 2, X1 - 2), chunks(4, 27), acc2, U2)
        between()
        with jax.named_scope(name + "_waitx"):
            wait_x()
        with jax.named_scope(name + "_ringx"):
            acc1 = first((X0 - 1, X0, X1 - 1, X1), chunks(2, 29), acc1)
            acc2 = second((X0, X0 + 1, X1 - 2, X1 - 1), chunks(4, 27), acc2)
        with jax.named_scope(name + "_waity"):
            wait_y()
        with jax.named_scope(name + "_ringy1"):
            acc1 = first((X0 - 1, X1), chunks(0, 1) + chunks(30, 31), acc1)
            acc1 = first(range(X0, X1), chunks(-2, 1) + chunks(30, 33), acc1, UY)
        with jax.named_scope(name + "_ringy2"):
            acc2 = second(range(X0, X1), chunks(0, 3) + chunks(28, 31), acc2, UY)
        return acc1, acc2

    own = chunks(0, 31)
    inner = chunks(2, 29)
    ends = chunks(0, 1) + chunks(30, 31)

    def own_weights(x, c, with_x=True, diagonal=True):
        for r in own:
            if with_x:
                weights_x(x, r)
            weights_z(x, r)
        for r in own[:-1]:
            weights_y(x, r)
        weights_y(x, R1 - 8, 4)
        if diagonal:
            for r in inner:
                add_diagonal(x, r)
        return c

    with jax.named_scope("weights1"):
        own_weights(X0, 0, diagonal=False)
        over(range(X0 + 1, X0 + 11), own_weights, 0, UW)
        for copy in loads[4:8]:
            copy.wait()
        exchange(1, up, 2, every_way)
    with jax.named_scope("weights2"):
        over(range(X0 + 11, X1 - 1), own_weights, 0, UW)
        own_weights(X1 - 1, 0, with_x=False, diagonal=False)
        for copy in loads[8:]:
            copy.wait()
        exchange(2, rb, 1, faces)

    def halo_weights():
        with jax.named_scope("wait_k"):
            arrived(0, kp, 2, every_way)
        with jax.named_scope("halo_weights"):
            for i in (X0 - 2, X0 - 1, X1 - 1, X1):
                for r in own:
                    weights_x(i, r)
            for x in (X0 - 1, X1):
                for r in own:
                    weights_z(x, r)
                    weights_y(x, r)
                weights_y(x, R0 - 4, 4)
                for r in own:
                    add_diagonal(x, r)
            for r in (R0 - 8, R1):
                weights_x(X0 - 1, r)

            def body(x, c):
                weights_y(x, R0 - 8, 8)
                weights_y(x, R1 - 4, 8)
                for r in (R0 - 8, R1):
                    weights_x(x, r)
                    weights_z(x, r)
                for r in (R0 - 8, R1) + ends:
                    add_diagonal(x, r)
                return c

            over(range(X0, X1), body, 0, UY)
            for x in (X0, X1 - 1):
                for r in inner:
                    add_diagonal(x, r)

    def wait_fields_x():
        arrived(1, up, 2, along_x)
        arrived(2, rb, 1, along_x)

    def wait_fields_y():
        arrived(1, up, 2, along_y + corners)
        arrived(2, rb, 1, along_y)

    pair = (zero, zero)
    (m0,), (m1, m2) = two_steps(
        "p1", step(up, rp, 1), step(rp, v1, 2), (zero,), pair, wait_fields_x, wait_fields_y, halo_weights
    )
    exchange(3, v1, 2, every_way)
    (m3, m4), (m5, m6) = two_steps(
        "p2", step(v1, v2, 2), step(v2, None, 2), pair, pair,
        lambda: arrived(3, v1, 2, along_x), lambda: arrived(3, v1, 2, along_y + corners), lambda: None,
    )
    moments = [m0, m1, m2, m3, m4, m5, m6]

    with jax.named_scope("moments"):
        stacked = zero
        for k, m in enumerate(moments):
            stacked = jnp.where(sub == k, jnp.sum(m, axis=0, keepdims=True), stacked)
        high, low = split_sum(stacked, 1)
        mine = jnp.sum(jnp.where(lane == sub, high, jnp.where(lane == sub + 8, low, 0.0)), axis=0, keepdims=True)
    place = gx * ngy + gy
    row[...] = mine
    gath[pl.ds(place, 1), :] = mine
    pl.semaphore_wait(ready, ngx - 1)
    with jax.named_scope("gsend"):
        for dx, dy in far_first(ngx, ngy):
            pltpu.make_async_remote_copy(
                src_ref=row, dst_ref=gath.at[pl.ds(place, 1), :], send_sem=gsend, recv_sem=grecv,
                device_id=(lax.rem(gx + dx, ngx), lax.rem(gy + dy, ngy)), device_id_type=MESH,
            ).start()
    every = pltpu.make_async_remote_copy(
        src_ref=gath.at[0 : count - 1, :], dst_ref=gath.at[0 : count - 1, :], send_sem=gsend, recv_sem=grecv,
        device_id=(gx, gy), device_id_type=MESH,
    )
    with jax.named_scope("gwait"):
        every.wait_recv()
    with jax.named_scope("solve"):
        high, low = split_sum(gath[...], 0)
        lane1 = lax.broadcasted_iota(jnp.int32, (1, 128), 1)

        def pick(v, k):
            return jnp.sum(jnp.where(lane1 == k, v, 0.0), axis=1, keepdims=True)

        m = [renorm(pick(high, k), pick(low, k) + pick(high + low, k + 8)) for k in range(7)]
        (y1, y2, y3), rest = normal_equations(m)
        est_ref[...] = jnp.broadcast_to(jnp.sqrt(jnp.maximum(rest, 0.0)), (1, 128))
        y1, y2, y3 = (jnp.broadcast_to(y, (8, 128)) for y in (y1, y2, y3))

    def combine(x, c):
        for r in own:
            s = slice(r, r + 8)
            sol_ref[x - X0, r - R0 : r - R0 + 8, :] = up[x, s, :] + (
                y1 * rp[x, s, :] + (y2 * v1[x, s, :] + y3 * v2[x, s, :])
            )
        return c

    with jax.named_scope("final"):
        over(range(X0, X1), combine, 0, 2)
    every.wait_send()
    sent(0, kp, 2, every_way)
    sent(1, up, 2, every_way)
    sent(2, rb, 1, faces)
    sent(3, v1, 2, every_way)


def local(ngx, ngy, right_side, start_guess, conductivity):
    field = pltpu.VMEM((PLANES, ROWS, 128), F32)
    sem = pltpu.SemaphoreType
    sol, est = pl.pallas_call(
        functools.partial(kernel, ngx, ngy),
        out_shape=(jax.ShapeDtypeStruct((32, 128, 128), F32), jax.ShapeDtypeStruct((1, 128), F32)),
        in_specs=[pl.BlockSpec(memory_space=pltpu.HBM)] * 3,
        out_specs=(pl.BlockSpec(memory_space=pltpu.VMEM), pl.BlockSpec(memory_space=pltpu.VMEM)),
        scratch_shapes=[field] * 11 + [
            pltpu.VMEM((1, 128), F32),
            pltpu.VMEM((ngx * ngy, 128), F32),
            sem.DMA((3, 4)), sem.DMA((4, 8)), sem.DMA((4, 8)), sem.DMA, sem.DMA, sem.REGULAR,
        ],
        compiler_params=pltpu.CompilerParams(
            collective_id=0, has_side_effects=True, vmem_limit_bytes=50 * 2**20
        ),
    )(right_side, start_guess, conductivity)
    return sol.reshape(32, 32, 512), est[0, 0]


def solution(mesh):
    return jax.shard_map(
        functools.partial(local, mesh.shape["gx"], mesh.shape["gy"]),
        mesh=mesh,
        in_specs=(P("gx", "gy", None),) * 3,
        out_specs=(P("gx", "gy", None), P()),
        check_vma=False,
    )
```

```python
import functools

import jax
import jax.numpy as jnp
from jax import lax
from jax.experimental import pallas as pl
from jax.experimental.pallas import tpu as pltpu
from jax.sharding import PartitionSpec as P

MESH = pl.DeviceIdType.MESH
F32 = jnp.float32
SCALE = 64.0
HALF = 0.5 / SCALE
X0, X1 = 3, 35
R0, R1 = 16, 144
PLANES, ROWS = 38, 160
UW, U1, U2, U3, UY = 5, 5, 4, 4, 8


def renorm(a, b):
    s = a + b
    return s, b - (s - a)


def two_sum(a, b):
    s = a + b
    t = s - a
    return s, (a - (s - t)) + (b - t)


def split(a):
    t = 4097.0 * a
    high = t - (t - a)
    return high, a - high


def two_prod(a, b):
    p = a * b
    (ah, al), (bh, bl) = split(a), split(b)
    return p, ((ah * bh - p) + ah * bl + al * bh) + al * bl


def add(a, b):
    s, e = two_sum(a[0], b[0])
    return renorm(s, e + (a[1] + b[1]))


def sub(a, b):
    return add(a, (-b[0], -b[1]))


def mul(a, b):
    p, e = two_prod(a[0], b[0])
    return renorm(p, e + (a[0] * b[1] + a[1] * b[0]))


def div(a, b):
    q = a[0] / b[0]
    p, e = two_prod(q, b[0])
    return renorm(q, (((a[0] - p) - e) + (a[1] - q * b[1])) / b[0])


def split_sum(v, axis):
    bound = 2.0 * jnp.sum(jnp.abs(v), axis=axis, keepdims=True)
    upper = (v + bound) - bound
    return jnp.sum(upper, axis=axis, keepdims=True), jnp.sum(v - upper, axis=axis, keepdims=True)


def normal_equations(m):
    l21, l31 = div(m[3], m[2]), div(m[4], m[2])
    d2 = sub(m[4], mul(l21, m[3]))
    e2 = sub(m[5], mul(l21, m[4]))
    l32 = div(e2, d2)
    d3 = sub(sub(m[6], mul(l31, m[4])), mul(l32, e2))
    c1 = m[1]
    c2 = sub(m[2], mul(l21, c1))
    c3 = sub(sub(m[3], mul(l31, c1)), mul(l32, c2))
    q1, q2, q3 = div(c1, m[2]), div(c2, d2), div(c3, d3)
    y3 = q3
    y2 = sub(q2, mul(l32, y3))
    y1 = sub(sub(q1, mul(l21, y2)), mul(l31, y3))
    rest = sub(sub(sub(m[0], mul(c1, q1)), mul(c2, q2)), mul(c3, q3))
    return tuple(y[0] / SCALE for y in (y1, y2, y3)), rest[0]


def directions(gx, gy, ngx, ngy):
    out = []
    for sx, sy in ((0, 1), (0, -1), (1, 0), (-1, 0), (1, 1), (1, -1), (-1, 1), (-1, -1)):
        to, come = [], []
        for step, at, n in ((sx, gx, ngx), (sy, gy, ngy)):
            if step:
                to.append(at < n - 1 if step > 0 else at > 0)
                come.append(at > 0 if step > 0 else at < n - 1)
        both = (lambda c: c[0]) if len(to) == 1 else (lambda c: jnp.logical_and(*c))
        out.append((sx, sy, both(to), both(come)))
    return out


def far_first(ngx, ngy):
    def ring(d):
        return min(d % 4, -d % 4)

    offsets = [(dx, dy) for dx in range(ngx) for dy in range(ngy) if dx or dy]
    return sorted(offsets, key=lambda o: -(ring(o[0] // 2) + ring(o[1] // 4) + ring(o[1] % 4)))


def extent(step, low, high, near, far, outside):
    if step == 0:
        return slice(low, high)
    if outside:
        return slice(low - far, low - near) if step > 0 else slice(high + near, high + far)
    return slice(high - far, high - near) if step > 0 else slice(low + near, low + far)


def piece(ref, sx, sy, layers, outside):
    near, far = (0, 2) if sx and sy else layers
    return ref.at[extent(sx, X0, X1, near, far, outside), extent(sy, R0, R1, 4 * near, 4 * far, outside), :]


def kernel(
    ngx, ngy,
    rhs_hbm, x0_hbm, k_hbm, sol_ref, est_ref,
    kp, up, rb, rp, v1, v2, wx, wy, wzm, wzp, dg, row, gath,
    load_sem, send_sem, recv_sem, gsend, grecv, ready,
):
    gx, gy = lax.axis_index("gx"), lax.axis_index("gy")
    count = ngx * ngy
    loads = []
    for i, (src, dst) in enumerate(((k_hbm, kp), (x0_hbm, up), (rhs_hbm, rb))):
        view = dst.reshape(PLANES, ROWS // 4, 4, 128)
        for q in range(4):
            loads.append(
                pltpu.make_async_copy(
                    src.at[:, :, q * 128 : (q + 1) * 128],
                    view.at[X0:X1, R0 // 4 : R1 // 4, q, :],
                    load_sem.at[i, q],
                )
            )
    for copy in loads:
        copy.start()

    barrier = pltpu.get_barrier_semaphore()
    greet = [(d, 0) for d in range(1, ngx)] + [(0, d) for d in range(1, ngy)]
    greet += [(1, 1), (1, ngy - 1), (ngx - 1, 1), (ngx - 1, ngy - 1)]
    for dx, dy in greet:
        pl.semaphore_signal(
            barrier, inc=1, device_id=(lax.rem(gx + dx, ngx), lax.rem(gy + dy, ngy)), device_id_type=MESH
        )

    dirs = directions(gx, gy, ngx, ngy)
    has_low_x, has_high_x, has_low_y, has_high_y = gx > 0, gx < ngx - 1, gy > 0, gy < ngy - 1
    fields = (kp, up, rp, v1, v2)
    zero = jnp.zeros((8, 128), F32)

    for at, inside in ((0, has_low_x), (X1, has_high_x)):

        @pl.when(jnp.logical_not(inside))
        def _():
            def fill(i, c):
                for f in fields:
                    for x in range(at, at + 3):
                        f[x, pl.ds(pl.multiple_of(8 * i, 8), 8), :] = zero
                return c

            lax.fori_loop(0, ROWS // 8, fill, 0)

    for at, inside in ((0, has_low_y), (R1, has_high_y)):

        @pl.when(jnp.logical_not(inside))
        def _():
            def fill(x, c):
                for f in fields:
                    for r in (at, at + 8):
                        f[x, r : r + 8, :] = zero
                return c

            lax.fori_loop(0, PLANES, fill, 0)

    def copy_of(e, f, layers, i):
        sx, sy = dirs[i][:2]
        return pltpu.make_async_remote_copy(
            src_ref=piece(f, sx, sy, layers, False), dst_ref=piece(f, sx, sy, layers, True),
            send_sem=send_sem.at[e, i], recv_sem=recv_sem.at[e, i],
            device_id={"gx": lax.rem(gx + sx + ngx, ngx), "gy": lax.rem(gy + sy + ngy, ngy)},
            device_id_type=MESH,
        )

    def exchange(e, f, layers, which):
        for i in which:

            @pl.when(dirs[i][2])
            def _():
                copy_of(e, f, layers, i).start()

    def arrived(e, f, layers, which):
        for i in which:

            @pl.when(dirs[i][3])
            def _():
                copy_of(e, f, layers, i).wait_recv()

    def sent(e, f, layers, which):
        for i in which:

            @pl.when(dirs[i][2])
            def _():
                copy_of(e, f, layers, i).wait_send()

    along_y, along_x, corners = (0, 1), (2, 3), (4, 5, 6, 7)
    every_way = corners + along_y + along_x
    faces = along_y + along_x

    with jax.named_scope("load_k"):
        for copy in loads[:4]:
            copy.wait()
    with jax.named_scope("barrier"):
        pl.semaphore_wait(barrier, len(greet))
        exchange(0, kp, (0, 1), faces)
        for d in range(1, ngx):
            pl.semaphore_signal(ready, inc=1, device_id=(lax.rem(gx + d, ngx), gy), device_id_type=MESH)

    lane = lax.broadcasted_iota(jnp.int32, (8, 128), 1)
    sub = lax.broadcasted_iota(jnp.int32, (8, 128), 0)
    zhi = lax.rem(sub, 4)
    first_lane, last_lane = lane == 0, lane == 127
    z_first = jnp.logical_and(first_lane, zhi == 0)
    z_last = jnp.logical_and(last_lane, zhi == 3)

    def z_up(f, x, r, centre):
        return pltpu.roll(jnp.where(first_lane, f[x, r + 1 : r + 9, :], centre), 127, 1)

    def z_down(f, x, r, centre):
        return pltpu.roll(jnp.where(last_lane, f[x, r - 1 : r + 7, :], centre), 1, 1)

    def weights_x(i, r):
        wx[i, r : r + 8, :] = HALF * (kp[i, r : r + 8, :] + kp[i + 1, r : r + 8, :])

    def weights_y(x, r, n=8):
        wy[x, r : r + n, :] = HALF * (kp[x, r : r + n, :] + kp[x, r + 4 : r + 4 + n, :])

    def weights_z(x, r):
        centre = kp[x, r : r + 8, :]
        above = jnp.where(first_lane, pltpu.roll(centre, 7, 0), centre)
        below = jnp.where(last_lane, pltpu.roll(centre, 1, 0), centre)
        up_w = HALF * (centre + jnp.where(z_last, 0.0, pltpu.roll(above, 127, 1)))
        down_w = HALF * (centre + jnp.where(z_first, 0.0, pltpu.roll(below, 1, 1)))
        dg[x, r : r + 8, :] = up_w + down_w
        wzp[x, r : r + 8, :] = jnp.where(z_last, 0.0, up_w)
        wzm[x, r : r + 8, :] = jnp.where(z_first, 0.0, down_w)

    def add_diagonal(x, r):
        s = slice(r, r + 8)
        dg[x, s, :] = dg[x, s, :] + ((wx[x - 1, s, :] + wx[x, s, :]) + (wy[x, r - 4 : r + 4, :] + wy[x, s, :]))

    def apply(f, x, r):
        s = slice(r, r + 8)
        centre = f[x, s, :]
        out = dg[x, s, :] * centre
        out = out - wx[x - 1, s, :] * f[x - 1, s, :]
        out = out - wx[x, s, :] * f[x + 1, s, :]
        out = out - wy[x, r - 4 : r + 4, :] * f[x, r - 4 : r + 4, :]
        out = out - wy[x, s, :] * f[x, r + 4 : r + 12, :]
        out = out - wzm[x, s, :] * z_down(f, x, r, centre)
        out = out - wzp[x, s, :] * z_up(f, x, r, centre)
        return centre, out

    def chunks(first, last, counts=None):
        return tuple((r, 3 if counts is None else counts) for r in range(R0 + 4 * first, R0 + 4 * last, 8))

    def over(planes, body, carry, unroll=1):
        if not isinstance(planes, range):
            for x in planes:
                carry = body(x, carry)
            return carry
        first, steps = planes.start, len(planes) // unroll

        def several(i, carry):
            for u in range(unroll):
                carry = body(first + i * unroll + u, carry)
            return carry

        return lax.fori_loop(0, steps, several, carry)

    def step(f, w, counted):
        def run(planes, rows, acc, unroll=1):
            def body(x, acc):
                own = (zero,) * counted
                for r, layers in rows:
                    centre, out = apply(f, x, r)
                    if f is up:
                        out = rb[x, r : r + 8, :] - SCALE * out
                    inside = True
                    for at, low, high, below, beyond in (
                        (x, X0, X1, has_low_x, has_high_x), (r, R0, R1, has_low_y, has_high_y)
                    ):
                        if isinstance(at, int) and not low <= at < high:
                            inside = False
                            out = jnp.where(below if at < low else beyond, out, 0.0)
                    if w is not None:
                        w[x, r : r + 8, :] = out
                    if not inside or layers == 0:
                        continue
                    terms = (out * out,) if counted == 1 else (centre * out, out * out)
                    if layers < 3:
                        terms = tuple(jnp.where((sub < 4) == (layers == 1), t, 0.0) for t in terms)
                    own = tuple(o + t for o, t in zip(own, terms))
                return tuple(a + o for a, o in zip(acc, own))

            return over(planes, body, acc, unroll)

        return run

    own = [r for r, _ in chunks(0, 31)]
    inner = [r for r, _ in chunks(2, 29)]
    ends = (R0, R1 - 8)
    outer = (R0 - 8, R1)

    def own_weights(x, c, with_x=True, diagonal=True):
        for r in own:
            if with_x:
                weights_x(x, r)
            weights_z(x, r)
        for r in own[:-1]:
            weights_y(x, r)
        weights_y(x, R1 - 8, 4)
        if diagonal:
            for r in inner:
                add_diagonal(x, r)
        return c

    with jax.named_scope("weights1"):
        own_weights(X0, 0, diagonal=False)
        over(range(X0 + 1, X0 + 11), own_weights, 0, UW)
        for copy in loads[4:8]:
            copy.wait()
        exchange(1, up, (0, 1), faces)
        exchange(2, kp, (1, 3), every_way)
    with jax.named_scope("weights2"):
        over(range(X0 + 11, X1 - 1), own_weights, 0, UW)
        own_weights(X1 - 1, 0, with_x=False, diagonal=False)
        for copy in loads[8:]:
            copy.wait()

    residual = step(up, rp, 1)
    m0 = (zero,)
    with jax.named_scope("p1_in"):
        m0 = residual(range(X0 + 1, X1 - 1), chunks(2, 29), m0, U1)
    with jax.named_scope("wait_k"):
        arrived(0, kp, (0, 1), faces)
    with jax.named_scope("edge_weights"):
        for r in own:
            weights_x(X0 - 1, r)
            weights_x(X1 - 1, r)

        def edge(x, c):
            weights_y(x, R0 - 4, 4)
            weights_y(x, R1 - 4, 4)
            for r in ends:
                add_diagonal(x, r)
            return c

        over(range(X0, X1), edge, 0, UY)
        for x in (X0, X1 - 1):
            for r in inner:
                add_diagonal(x, r)
    with jax.named_scope("p1_waitx"):
        arrived(1, up, (0, 1), along_x)
    with jax.named_scope("p1_ringx"):
        m0 = residual((X0, X1 - 1), chunks(2, 29), m0)
    with jax.named_scope("p1_waity"):
        arrived(1, up, (0, 1), along_y)
    with jax.named_scope("p1_ringy"):
        m0 = residual(range(X0, X1), chunks(0, 1) + chunks(30, 31), m0, UY)
        exchange(3, rp, (0, 3), every_way)

    powers = (step(rp, v1, 2), step(v1, v2, 2), step(v2, None, 2))
    rows = (chunks(1, 30), chunks(2, 29), chunks(3, 28))
    acc = [(zero, zero)] * 3
    depth = (1, 2, 4)
    for n in range(3):
        with jax.named_scope("p2_in%d" % n):
            acc[n] = powers[n](range(X0 + depth[n], X1 - depth[n]), rows[n], acc[n], (U1, U2, U3)[n])
    with jax.named_scope("wait_k2"):
        arrived(2, kp, (1, 3), every_way)
    with jax.named_scope("halo_weights"):
        beside = (X0 - 2, X0 - 1, X1, X1 + 1)
        for i in (X0 - 3, X0 - 2, X1, X1 + 1):
            for r in own:
                weights_x(i, r)
        for x in beside:
            for r in own:
                weights_z(x, r)
                weights_y(x, r)
            weights_y(x, R0 - 4, 4)
            for r in own:
                add_diagonal(x, r)

        def halo(x, c, with_x=True):
            weights_y(x, R0 - 12, 8)
            weights_y(x, R1, 8)
            for r in outer:
                weights_x(x, r)
                weights_z(x, r)
                add_diagonal(x, r)
            return c

        for r in outer:
            weights_x(X0 - 2, r)
        halo(X0 - 1, 0)
        over(range(X0, X1), halo, 0, UY)
        halo(X1, 0)
    with jax.named_scope("p2_waitx"):
        arrived(3, rp, (0, 3), along_x)
    with jax.named_scope("p2_ringx"):
        for n in range(3):
            low, high = X0 - 2 + n, X1 + 2 - n
            acc[n] = powers[n](tuple(range(low, X0 + depth[n])) + tuple(range(X1 - depth[n], high)), rows[n], acc[n])
    with jax.named_scope("p2_waity"):
        arrived(3, rp, (0, 3), along_y + corners)
    halos = chunks(-2, -1, 0) + chunks(32, 33, 0)
    with jax.named_scope("p2_ringy0"):
        lines = chunks(0, 1, 1) + chunks(30, 31, 2)
        acc[0] = powers[0](beside, lines, acc[0])
        acc[0] = powers[0]((X0 - 1, X1), halos, acc[0])
        acc[0] = powers[0](range(X0, X1), lines + halos, acc[0], UY)
    with jax.named_scope("p2_ringy1"):
        lines = chunks(0, 1) + chunks(30, 31)
        acc[1] = powers[1]((X0 - 1, X1), lines, acc[1])
        acc[1] = powers[1](range(X0, X1), lines + halos, acc[1], UY)
    with jax.named_scope("p2_ringy2"):
        lines = chunks(0, 1) + chunks(2, 3, 1) + chunks(28, 29, 2) + chunks(30, 31)
        acc[2] = powers[2](range(X0, X1), lines, acc[2], UY)
    (m1, m2), (m3, m4), (m5, m6) = acc
    m0 = m0[0]
    moments = [m0, m1, m2, m3, m4, m5, m6]

    with jax.named_scope("moments"):
        stacked = zero
        for k, m in enumerate(moments):
            stacked = jnp.where(sub == k, jnp.sum(m, axis=0, keepdims=True), stacked)
        high, low = split_sum(stacked, 1)
        mine = jnp.sum(jnp.where(lane == sub, high, jnp.where(lane == sub + 8, low, 0.0)), axis=0, keepdims=True)
    place = gx * ngy + gy
    row[...] = mine
    gath[pl.ds(place, 1), :] = mine
    pl.semaphore_wait(ready, ngx - 1)
    with jax.named_scope("gsend"):
        for dx, dy in far_first(ngx, ngy):
            pltpu.make_async_remote_copy(
                src_ref=row, dst_ref=gath.at[pl.ds(place, 1), :], send_sem=gsend, recv_sem=grecv,
                device_id=(lax.rem(gx + dx, ngx), lax.rem(gy + dy, ngy)), device_id_type=MESH,
            ).start()
    every = pltpu.make_async_remote_copy(
        src_ref=gath.at[0 : count - 1, :], dst_ref=gath.at[0 : count - 1, :], send_sem=gsend, recv_sem=grecv,
        device_id=(gx, gy), device_id_type=MESH,
    )
    with jax.named_scope("gwait"):
        every.wait_recv()
    with jax.named_scope("solve"):
        high, low = split_sum(gath[...], 0)
        lane1 = lax.broadcasted_iota(jnp.int32, (1, 128), 1)

        def pick(v, k):
            return jnp.sum(jnp.where(lane1 == k, v, 0.0), axis=1, keepdims=True)

        m = [renorm(pick(high, k), pick(low, k) + pick(high + low, k + 8)) for k in range(7)]
        (y1, y2, y3), rest = normal_equations(m)
        est_ref[...] = jnp.broadcast_to(jnp.sqrt(jnp.maximum(rest, 0.0)), (1, 128))
        y1, y2, y3 = (jnp.broadcast_to(y, (8, 128)) for y in (y1, y2, y3))

    def combine(x, c):
        for r in own:
            s = slice(r, r + 8)
            sol_ref[x - X0, r - R0 : r - R0 + 8, :] = up[x, s, :] + (
                y1 * rp[x, s, :] + (y2 * v1[x, s, :] + y3 * v2[x, s, :])
            )
        return c

    with jax.named_scope("final"):
        over(range(X0, X1), combine, 0, 2)
    every.wait_send()
    sent(0, kp, (0, 1), faces)
    sent(1, up, (0, 1), faces)
    sent(2, kp, (1, 3), every_way)
    sent(3, rp, (0, 3), every_way)


def local(ngx, ngy, right_side, start_guess, conductivity):
    field = pltpu.VMEM((PLANES, ROWS, 128), F32)
    sem = pltpu.SemaphoreType
    sol, est = pl.pallas_call(
        functools.partial(kernel, ngx, ngy),
        out_shape=(jax.ShapeDtypeStruct((32, 128, 128), F32), jax.ShapeDtypeStruct((1, 128), F32)),
        in_specs=[pl.BlockSpec(memory_space=pltpu.HBM)] * 3,
        out_specs=(pl.BlockSpec(memory_space=pltpu.VMEM), pl.BlockSpec(memory_space=pltpu.VMEM)),
        scratch_shapes=[field] * 11 + [
            pltpu.VMEM((1, 128), F32),
            pltpu.VMEM((ngx * ngy, 128), F32),
            sem.DMA((3, 4)), sem.DMA((4, 8)), sem.DMA((4, 8)), sem.DMA, sem.DMA, sem.REGULAR,
        ],
        compiler_params=pltpu.CompilerParams(
            collective_id=0, has_side_effects=True, vmem_limit_bytes=50 * 2**20
        ),
    )(right_side, start_guess, conductivity)
    return sol.reshape(32, 32, 512), est[0, 0]


def solution(mesh):
    return jax.shard_map(
        functools.partial(local, mesh.shape["gx"], mesh.shape["gy"]),
        mesh=mesh,
        in_specs=(P("gx", "gy", None),) * 3,
        out_specs=(P("gx", "gy", None), P()),
        check_vma=False,
    )
```

```python
import functools

import jax
import jax.numpy as jnp
from jax import lax
from jax.experimental import pallas as pl
from jax.experimental.pallas import tpu as pltpu
from jax.sharding import PartitionSpec as P

MESH = pl.DeviceIdType.MESH
F32 = jnp.float32
SCALE = 64.0
HALF = 0.5 / SCALE
X0, X1 = 3, 35
R0, R1 = 16, 144
PLANES, ROWS = 38, 160
UW, U1, U2, U3, UY = 5, 5, 4, 4, 8


def renorm(a, b):
    s = a + b
    return s, b - (s - a)


def two_sum(a, b):
    s = a + b
    t = s - a
    return s, (a - (s - t)) + (b - t)


def split(a):
    t = 4097.0 * a
    high = t - (t - a)
    return high, a - high


def two_prod(a, b):
    p = a * b
    (ah, al), (bh, bl) = split(a), split(b)
    return p, ((ah * bh - p) + ah * bl + al * bh) + al * bl


def add(a, b):
    s, e = two_sum(a[0], b[0])
    return renorm(s, e + (a[1] + b[1]))


def sub(a, b):
    return add(a, (-b[0], -b[1]))


def mul(a, b):
    p, e = two_prod(a[0], b[0])
    return renorm(p, e + (a[0] * b[1] + a[1] * b[0]))


def div(a, b):
    q = a[0] / b[0]
    p, e = two_prod(q, b[0])
    return renorm(q, (((a[0] - p) - e) + (a[1] - q * b[1])) / b[0])


def split_sum(v, axis):
    bound = 2.0 * jnp.sum(jnp.abs(v), axis=axis, keepdims=True)
    upper = (v + bound) - bound
    return jnp.sum(upper, axis=axis, keepdims=True), jnp.sum(v - upper, axis=axis, keepdims=True)


def normal_equations(m):
    l21, l31 = div(m[3], m[2]), div(m[4], m[2])
    d2 = sub(m[4], mul(l21, m[3]))
    e2 = sub(m[5], mul(l21, m[4]))
    l32 = div(e2, d2)
    d3 = sub(sub(m[6], mul(l31, m[4])), mul(l32, e2))
    c1 = m[1]
    c2 = sub(m[2], mul(l21, c1))
    c3 = sub(sub(m[3], mul(l31, c1)), mul(l32, c2))
    q1, q2, q3 = div(c1, m[2]), div(c2, d2), div(c3, d3)
    y3 = q3
    y2 = sub(q2, mul(l32, y3))
    y1 = sub(sub(q1, mul(l21, y2)), mul(l31, y3))
    rest = sub(sub(sub(m[0], mul(c1, q1)), mul(c2, q2)), mul(c3, q3))
    return tuple(y[0] / SCALE for y in (y1, y2, y3)), rest[0]


def directions(gx, gy, ngx, ngy):
    out = []
    for sx, sy in ((0, 1), (0, -1), (1, 0), (-1, 0), (1, 1), (1, -1), (-1, 1), (-1, -1)):
        to, come = [], []
        for step, at, n in ((sx, gx, ngx), (sy, gy, ngy)):
            if step:
                to.append(at < n - 1 if step > 0 else at > 0)
                come.append(at > 0 if step > 0 else at < n - 1)
        both = (lambda c: c[0]) if len(to) == 1 else (lambda c: jnp.logical_and(*c))
        out.append((sx, sy, both(to), both(come)))
    return out


def far_first(ngx, ngy):
    def ring(d):
        return min(d % 4, -d % 4)

    offsets = [(dx, dy) for dx in range(ngx) for dy in range(ngy) if dx or dy]
    return sorted(offsets, key=lambda o: -(ring(o[0] // 2) + ring(o[1] // 4) + ring(o[1] % 4)))


def extent(step, low, high, near, far, outside):
    if step == 0:
        return slice(low, high)
    if outside:
        return slice(low - far, low - near) if step > 0 else slice(high + near, high + far)
    return slice(high - far, high - near) if step > 0 else slice(low + near, low + far)


def piece(ref, sx, sy, layers, outside):
    near, far = (0, 2) if sx and sy else layers
    return ref.at[extent(sx, X0, X1, near, far, outside), extent(sy, R0, R1, 4 * near, 4 * far, outside), :]


def kernel(
    ngx, ngy,
    rhs_hbm, x0_hbm, k_hbm, sol_ref, est_ref,
    kp, up, rb, rp, v1, v2, wx, wy, wzm, wzp, dg, row, gath,
    load_sem, send_sem, recv_sem, gsend, grecv, ready,
):
    gx, gy = lax.axis_index("gx"), lax.axis_index("gy")
    xs, ys = [lax.rem(gx + d, ngx) for d in range(ngx)], [lax.rem(gy + d, ngy) for d in range(ngy)]
    barrier = pltpu.get_barrier_semaphore()
    near = [(0, 1), (0, ngy - 1), (1, 0), (ngx - 1, 0), (1, 1), (1, ngy - 1), (ngx - 1, 1), (ngx - 1, ngy - 1)]
    greet = near + [(d, 0) for d in range(2, ngx - 1)] + [(0, d) for d in range(2, ngy - 1)]
    for dx, dy in greet:
        pl.semaphore_signal(
            barrier, inc=1, device_id=(xs[dx], ys[dy]), device_id_type=MESH
        )
    count = ngx * ngy
    loads = []
    for i, (src, dst) in enumerate(((k_hbm, kp), (x0_hbm, up), (rhs_hbm, rb))):
        view = dst.reshape(PLANES, ROWS // 4, 4, 128)
        for q in range(4):
            loads.append(
                pltpu.make_async_copy(
                    src.at[:, :, q * 128 : (q + 1) * 128],
                    view.at[X0:X1, R0 // 4 : R1 // 4, q, :],
                    load_sem.at[i, q],
                )
            )
    for copy in loads[:8]:
        copy.start()
    dirs = directions(gx, gy, ngx, ngy)
    has_low_x, has_high_x, has_low_y, has_high_y = gx > 0, gx < ngx - 1, gy > 0, gy < ngy - 1
    fields = (kp, up, rp, v1, v2)
    zero = jnp.zeros((8, 128), F32)

    for at, inside in ((0, has_low_x), (X1, has_high_x)):

        @pl.when(jnp.logical_not(inside))
        def _():
            def fill(i, c):
                for f in fields:
                    for x in range(at, at + 3):
                        f[x, pl.ds(pl.multiple_of(8 * i, 8), 8), :] = zero
                return c

            lax.fori_loop(0, ROWS // 8, fill, 0)

    for at, inside in ((0, has_low_y), (R1, has_high_y)):

        @pl.when(jnp.logical_not(inside))
        def _():
            def fill(x, c):
                for f in fields:
                    for r in (at, at + 8):
                        f[x, r : r + 8, :] = zero
                return c

            lax.fori_loop(0, PLANES, fill, 0)

    def copy_of(e, f, layers, i):
        sx, sy = dirs[i][:2]
        return pltpu.make_async_remote_copy(
            src_ref=piece(f, sx, sy, layers, False), dst_ref=piece(f, sx, sy, layers, True),
            send_sem=send_sem.at[e, i], recv_sem=recv_sem.at[e, i],
            device_id={"gx": lax.rem(gx + sx + ngx, ngx), "gy": lax.rem(gy + sy + ngy, ngy)},
            device_id_type=MESH,
        )

    def exchange(e, f, layers, which):
        for i in which:

            @pl.when(dirs[i][2])
            def _():
                copy_of(e, f, layers, i).start()

    def arrived(e, f, layers, which):
        for i in which:

            @pl.when(dirs[i][3])
            def _():
                copy_of(e, f, layers, i).wait_recv()

    def sent(e, f, layers, which):
        for i in which:

            @pl.when(dirs[i][2])
            def _():
                copy_of(e, f, layers, i).wait_send()

    along_y, along_x, corners = (0, 1), (2, 3), (4, 5, 6, 7)
    every_way = corners + along_y + along_x
    faces = along_y + along_x

    with jax.named_scope("load_k"):
        for copy in loads[:4]:
            copy.wait()
        for copy in loads[8:]:
            copy.start()
    with jax.named_scope("barrier"):
        pl.semaphore_wait(barrier, len(greet))
        exchange(0, kp, (0, 1), faces)
        for d in range(1, ngx):
            pl.semaphore_signal(ready, inc=1, device_id=(lax.rem(gx + d, ngx), gy), device_id_type=MESH)

    lane = lax.broadcasted_iota(jnp.int32, (8, 128), 1)
    sub = lax.broadcasted_iota(jnp.int32, (8, 128), 0)
    zhi = lax.rem(sub, 4)
    first_lane, last_lane = lane == 0, lane == 127
    z_first = jnp.logical_and(first_lane, zhi == 0)
    z_last = jnp.logical_and(last_lane, zhi == 3)

    def z_up(f, x, r, centre):
        return pltpu.roll(jnp.where(first_lane, f[x, r + 1 : r + 9, :], centre), 127, 1)

    def z_down(f, x, r, centre):
        return pltpu.roll(jnp.where(last_lane, f[x, r - 1 : r + 7, :], centre), 1, 1)

    def weights_x(i, r):
        wx[i, r : r + 8, :] = HALF * (kp[i, r : r + 8, :] + kp[i + 1, r : r + 8, :])

    def weights_y(x, r, n=8):
        wy[x, r : r + n, :] = HALF * (kp[x, r : r + n, :] + kp[x, r + 4 : r + 4 + n, :])

    def weights_z(x, r):
        centre = kp[x, r : r + 8, :]
        above = jnp.where(first_lane, pltpu.roll(centre, 7, 0), centre)
        below = jnp.where(last_lane, pltpu.roll(centre, 1, 0), centre)
        up_w = HALF * (centre + jnp.where(z_last, 0.0, pltpu.roll(above, 127, 1)))
        down_w = HALF * (centre + jnp.where(z_first, 0.0, pltpu.roll(below, 1, 1)))
        dg[x, r : r + 8, :] = up_w + down_w
        wzp[x, r : r + 8, :] = jnp.where(z_last, 0.0, up_w)
        wzm[x, r : r + 8, :] = jnp.where(z_first, 0.0, down_w)

    def add_diagonal(x, r):
        s = slice(r, r + 8)
        dg[x, s, :] = dg[x, s, :] + ((wx[x - 1, s, :] + wx[x, s, :]) + (wy[x, r - 4 : r + 4, :] + wy[x, s, :]))

    def apply(f, x, r):
        s = slice(r, r + 8)
        centre = f[x, s, :]
        out = dg[x, s, :] * centre
        out = out - wx[x - 1, s, :] * f[x - 1, s, :]
        out = out - wx[x, s, :] * f[x + 1, s, :]
        out = out - wy[x, r - 4 : r + 4, :] * f[x, r - 4 : r + 4, :]
        out = out - wy[x, s, :] * f[x, r + 4 : r + 12, :]
        out = out - wzm[x, s, :] * z_down(f, x, r, centre)
        out = out - wzp[x, s, :] * z_up(f, x, r, centre)
        return centre, out

    def chunks(first, last, counts=None):
        return tuple((r, 3 if counts is None else counts) for r in range(R0 + 4 * first, R0 + 4 * last, 8))

    def over(planes, body, carry, unroll=1):
        if not isinstance(planes, range):
            for x in planes:
                carry = body(x, carry)
            return carry
        first, steps = planes.start, len(planes) // unroll

        def several(i, carry):
            for u in range(unroll):
                carry = body(first + i * unroll + u, carry)
            return carry

        return lax.fori_loop(0, steps, several, carry)

    def step(f, w, counted):
        def run(planes, rows, acc, unroll=1):
            def body(x, acc):
                own = (zero,) * counted
                for r, layers in rows:
                    centre, out = apply(f, x, r)
                    if f is up:
                        out = rb[x, r : r + 8, :] - SCALE * out
                    inside = True
                    for at, low, high, below, beyond in (
                        (x, X0, X1, has_low_x, has_high_x), (r, R0, R1, has_low_y, has_high_y)
                    ):
                        if isinstance(at, int) and not low <= at < high:
                            inside = False
                            out = jnp.where(below if at < low else beyond, out, 0.0)
                    if w is not None:
                        w[x, r : r + 8, :] = out
                    if not inside or layers == 0:
                        continue
                    terms = (out * out,) if counted == 1 else (centre * out, out * out)
                    if layers < 3:
                        terms = tuple(jnp.where((sub < 4) == (layers == 1), t, 0.0) for t in terms)
                    own = tuple(o + t for o, t in zip(own, terms))
                return tuple(a + o for a, o in zip(acc, own))

            return over(planes, body, acc, unroll)

        return run

    own = [r for r, _ in chunks(0, 31)]
    inner = [r for r, _ in chunks(2, 29)]
    ends = (R0, R1 - 8)
    outer = (R0 - 8, R1)

    def own_weights(x, c, with_x=True, diagonal=True):
        for r in own:
            if with_x:
                weights_x(x, r)
            weights_z(x, r)
        for r in own[:-1]:
            weights_y(x, r)
        weights_y(x, R1 - 8, 4)
        if diagonal:
            for r in inner:
                add_diagonal(x, r)
        return c

    with jax.named_scope("weights1"):
        own_weights(X0, 0, diagonal=False)
        over(range(X0 + 1, X0 + 11), own_weights, 0, UW)
        for copy in loads[4:8]:
            copy.wait()
        exchange(1, up, (0, 1), faces)
        exchange(2, kp, (1, 3), every_way)
    with jax.named_scope("weights2"):
        over(range(X0 + 11, X1 - 1), own_weights, 0, UW)
        own_weights(X1 - 1, 0, with_x=False, diagonal=False)
        for copy in loads[8:]:
            copy.wait()

    residual = step(up, rp, 1)
    m0 = (zero,)
    with jax.named_scope("p1_in"):
        m0 = residual(range(X0 + 1, X1 - 1), chunks(2, 29), m0, U1)
    with jax.named_scope("wait_k"):
        arrived(0, kp, (0, 1), faces)
    with jax.named_scope("edge_weights"):
        for r in own:
            weights_x(X0 - 1, r)
            weights_x(X1 - 1, r)

        def edge(x, c):
            weights_y(x, R0 - 4, 4)
            weights_y(x, R1 - 4, 4)
            for r in ends:
                add_diagonal(x, r)
            return c

        over(range(X0, X1), edge, 0, UY)
        for x in (X0, X1 - 1):
            for r in inner:
                add_diagonal(x, r)
    with jax.named_scope("p1_waitx"):
        arrived(1, up, (0, 1), along_x)
    with jax.named_scope("p1_ringx"):
        m0 = residual((X0, X1 - 1), chunks(2, 29), m0)
    high_last = lax.rem(gy, 4) == 3
    sides = (((0,), (5, 7), chunks(0, 1)), ((1,), (4, 6), chunks(30, 31)))

    def residual_strips(order):
        def run(m0):
            for side in order:
                with jax.named_scope("p1_waity%d" % side):
                    arrived(1, up, (0, 1), sides[side][0])
                with jax.named_scope("p1_ringy%d" % side):
                    m0 = residual(tuple(range(X0, X1)), sides[side][2], m0)
                    exchange(3, rp, (0, 3), sides[side][1] + (1 - side,))
            return m0

        return run

    m0 = lax.cond(high_last, residual_strips((0, 1)), residual_strips((1, 0)), m0)
    exchange(3, rp, (0, 3), along_x)

    powers = (step(rp, v1, 2), step(v1, v2, 2), step(v2, None, 2))
    rows = (chunks(1, 30), chunks(2, 29), chunks(3, 28))
    acc = [(zero, zero)] * 3
    depth = (1, 2, 4)
    for n in range(3):
        with jax.named_scope("p2_in%d" % n):
            acc[n] = powers[n](range(X0 + depth[n], X1 - depth[n]), rows[n], acc[n], (U1, U2, U3)[n])
    with jax.named_scope("wait_k2"):
        arrived(2, kp, (1, 3), every_way)
    with jax.named_scope("halo_weights"):
        beside = (X0 - 2, X0 - 1, X1, X1 + 1)
        for i in (X0 - 3, X0 - 2, X1, X1 + 1):
            for r in own:
                weights_x(i, r)
        for x in beside:
            for r in own:
                weights_z(x, r)
                weights_y(x, r)
            weights_y(x, R0 - 4, 4)
            for r in own:
                add_diagonal(x, r)

        def halo(x, c, with_x=True):
            weights_y(x, R0 - 12, 8)
            weights_y(x, R1, 8)
            for r in outer:
                weights_x(x, r)
                weights_z(x, r)
                add_diagonal(x, r)
            return c

        for r in outer:
            weights_x(X0 - 2, r)
        halo(X0 - 1, 0)
        over(range(X0, X1), halo, 0, UY)
        halo(X1, 0)
    with jax.named_scope("p2_waitx"):
        arrived(3, rp, (0, 3), along_x)
    with jax.named_scope("p2_ringx"):
        for n in range(3):
            low, high = X0 - 2 + n, X1 + 2 - n
            acc[n] = powers[n](tuple(range(low, X0 + depth[n])) + tuple(range(X1 - depth[n], high)), rows[n], acc[n])
    strips = (
        ((0, 4, 6), chunks(0, 1, 1), chunks(-2, -1, 0), chunks(0, 1), chunks(0, 1) + chunks(2, 3, 1)),
        ((1, 5, 7), chunks(30, 31, 2), chunks(32, 33, 0), chunks(30, 31), chunks(28, 29, 2) + chunks(30, 31)),
    )

    def power_strips(order):
        def run(acc):
            acc = list(acc)
            for side in order:
                ways, line, halos, line1, line2 = strips[side]
                with jax.named_scope("p2_waity%d" % side):
                    arrived(3, rp, (0, 3), ways)
                with jax.named_scope("p2_ringy%d" % side):
                    acc[0] = powers[0](beside, line, acc[0])
                    acc[0] = powers[0]((X0 - 1, X1), halos, acc[0])
                    acc[0] = powers[0](tuple(range(X0, X1)), line + halos, acc[0])
                    acc[1] = powers[1]((X0 - 1, X1), line1, acc[1])
                    acc[1] = powers[1](tuple(range(X0, X1)), line1 + halos, acc[1])
                    acc[2] = powers[2](tuple(range(X0, X1)), line2, acc[2])
            return tuple(acc)

        return run

    acc = lax.cond(high_last, power_strips((0, 1)), power_strips((1, 0)), tuple(acc))
    (m1, m2), (m3, m4), (m5, m6) = acc
    m0 = m0[0]
    moments = [m0, m1, m2, m3, m4, m5, m6]

    with jax.named_scope("moments"):
        stacked = zero
        for k, m in enumerate(moments):
            stacked = jnp.where(sub == k, jnp.sum(m, axis=0, keepdims=True), stacked)
        high, low = split_sum(stacked, 1)
        mine = jnp.sum(jnp.where(lane == sub, high, jnp.where(lane == sub + 8, low, 0.0)), axis=0, keepdims=True)
    place = gx * ngy + gy
    row[...] = mine
    gath[pl.ds(place, 1), :] = mine
    pl.semaphore_wait(ready, ngx - 1)
    with jax.named_scope("gsend"):
        for dx, dy in far_first(ngx, ngy):
            pltpu.make_async_remote_copy(
                src_ref=row, dst_ref=gath.at[pl.ds(place, 1), :], send_sem=gsend, recv_sem=grecv,
                device_id=(xs[dx], ys[dy]), device_id_type=MESH,
            ).start()
    every = pltpu.make_async_remote_copy(
        src_ref=gath.at[0 : count - 1, :], dst_ref=gath.at[0 : count - 1, :], send_sem=gsend, recv_sem=grecv,
        device_id=(gx, gy), device_id_type=MESH,
    )
    with jax.named_scope("gwait"):
        every.wait_recv()
    with jax.named_scope("solve"):
        high, low = split_sum(gath[...], 0)
        lane1 = lax.broadcasted_iota(jnp.int32, (1, 128), 1)

        def pick(v, k):
            return jnp.sum(jnp.where(lane1 == k, v, 0.0), axis=1, keepdims=True)

        m = [renorm(pick(high, k), pick(low, k) + pick(high + low, k + 8)) for k in range(7)]
        (y1, y2, y3), rest = normal_equations(m)
        est_ref[...] = jnp.broadcast_to(jnp.sqrt(jnp.maximum(rest, 0.0)), (1, 128))
        y1, y2, y3 = (jnp.broadcast_to(y, (8, 128)) for y in (y1, y2, y3))

    def combine(x, c):
        for y in range(0, 32, 8):
            for q in range(4):
                s = pl.ds(R0 + 4 * y + q, 8, stride=4)
                sol_ref[x - X0, y : y + 8, q * 128 : (q + 1) * 128] = up[x, s, :] + (
                    y1 * rp[x, s, :] + (y2 * v1[x, s, :] + y3 * v2[x, s, :])
                )
        return c

    with jax.named_scope("final"):
        over(range(X0, X1), combine, 0, 2)
    every.wait_send()
    sent(0, kp, (0, 1), faces)
    sent(1, up, (0, 1), faces)
    sent(2, kp, (1, 3), every_way)
    sent(3, rp, (0, 3), every_way)


def local(ngx, ngy, right_side, start_guess, conductivity):
    field = pltpu.VMEM((PLANES, ROWS, 128), F32)
    sem = pltpu.SemaphoreType
    sol, est = pl.pallas_call(
        functools.partial(kernel, ngx, ngy),
        out_shape=(jax.ShapeDtypeStruct((32, 32, 512), F32), jax.ShapeDtypeStruct((1, 128), F32)),
        in_specs=[pl.BlockSpec(memory_space=pltpu.HBM)] * 3,
        out_specs=(pl.BlockSpec(memory_space=pltpu.VMEM), pl.BlockSpec(memory_space=pltpu.VMEM)),
        scratch_shapes=[field] * 11 + [
            pltpu.VMEM((1, 128), F32),
            pltpu.VMEM((ngx * ngy, 128), F32),
            sem.DMA((3, 4)), sem.DMA((4, 8)), sem.DMA((4, 8)), sem.DMA, sem.DMA, sem.REGULAR,
        ],
        compiler_params=pltpu.CompilerParams(
            collective_id=0, has_side_effects=True, vmem_limit_bytes=50 * 2**20
        ),
    )(right_side, start_guess, conductivity)
    return sol, est[0, 0]


def solution(mesh):
    return jax.shard_map(
        functools.partial(local, mesh.shape["gx"], mesh.shape["gy"]),
        mesh=mesh,
        in_specs=(P("gx", "gy", None),) * 3,
        out_specs=(P("gx", "gy", None), P()),
        check_vma=False,
    )
```

```python
import functools

import jax
import jax.numpy as jnp
from jax import lax
from jax.experimental import pallas as pl
from jax.experimental.pallas import tpu as pltpu
from jax.sharding import PartitionSpec as P

MESH = pl.DeviceIdType.MESH
F32 = jnp.float32
SCALE = 64.0
HALF = 0.5 / SCALE
X0, X1 = 3, 35
R0, R1 = 16, 144
PLANES, ROWS = 38, 160
UW, U1, U2, U3, UY = 5, 5, 4, 4, 8


def renorm(a, b):
    s = a + b
    return s, b - (s - a)


def two_sum(a, b):
    s = a + b
    t = s - a
    return s, (a - (s - t)) + (b - t)


def split(a):
    t = 4097.0 * a
    high = t - (t - a)
    return high, a - high


def two_prod(a, b):
    p = a * b
    (ah, al), (bh, bl) = split(a), split(b)
    return p, ((ah * bh - p) + ah * bl + al * bh) + al * bl


def add(a, b):
    s, e = two_sum(a[0], b[0])
    return renorm(s, e + (a[1] + b[1]))


def sub(a, b):
    return add(a, (-b[0], -b[1]))


def mul(a, b):
    p, e = two_prod(a[0], b[0])
    return renorm(p, e + (a[0] * b[1] + a[1] * b[0]))


def div(a, b):
    q = a[0] / b[0]
    p, e = two_prod(q, b[0])
    return renorm(q, (((a[0] - p) - e) + (a[1] - q * b[1])) / b[0])


def split_sum(v, axis):
    bound = 2.0 * jnp.sum(jnp.abs(v), axis=axis, keepdims=True)
    upper = (v + bound) - bound
    return jnp.sum(upper, axis=axis, keepdims=True), jnp.sum(v - upper, axis=axis, keepdims=True)


def normal_equations(m):
    l21, l31 = div(m[3], m[2]), div(m[4], m[2])
    d2 = sub(m[4], mul(l21, m[3]))
    e2 = sub(m[5], mul(l21, m[4]))
    l32 = div(e2, d2)
    d3 = sub(sub(m[6], mul(l31, m[4])), mul(l32, e2))
    c1 = m[1]
    c2 = sub(m[2], mul(l21, c1))
    c3 = sub(sub(m[3], mul(l31, c1)), mul(l32, c2))
    q1, q2, q3 = div(c1, m[2]), div(c2, d2), div(c3, d3)
    y3 = q3
    y2 = sub(q2, mul(l32, y3))
    y1 = sub(sub(q1, mul(l21, y2)), mul(l31, y3))
    rest = sub(sub(sub(m[0], mul(c1, q1)), mul(c2, q2)), mul(c3, q3))
    return tuple(y[0] / SCALE for y in (y1, y2, y3)), rest[0]


def directions(gx, gy, ngx, ngy):
    out = []
    for sx, sy in ((0, 1), (0, -1), (1, 0), (-1, 0), (1, 1), (1, -1), (-1, 1), (-1, -1)):
        to, come = [], []
        for step, at, n in ((sx, gx, ngx), (sy, gy, ngy)):
            if step:
                to.append(at < n - 1 if step > 0 else at > 0)
                come.append(at > 0 if step > 0 else at < n - 1)
        both = (lambda c: c[0]) if len(to) == 1 else (lambda c: jnp.logical_and(*c))
        out.append((sx, sy, both(to), both(come)))
    return out


def far_first(ngx, ngy):
    def ring(d):
        return min(d % 4, -d % 4)

    offsets = [(dx, dy) for dx in range(ngx) for dy in range(ngy) if dx or dy]
    return sorted(offsets, key=lambda o: -(ring(o[0] // 2) + ring(o[1] // 4) + ring(o[1] % 4)))


def extent(step, low, high, near, far, outside):
    if step == 0:
        return slice(low, high)
    if outside:
        return slice(low - far, low - near) if step > 0 else slice(high + near, high + far)
    return slice(high - far, high - near) if step > 0 else slice(low + near, low + far)


def piece(ref, sx, sy, layers, outside):
    near, far = (0, 2) if sx and sy else layers
    return ref.at[extent(sx, X0, X1, near, far, outside), extent(sy, R0, R1, 4 * near, 4 * far, outside), :]


def kernel(
    ngx, ngy,
    rhs_hbm, x0_hbm, k_hbm, sol_ref, est_ref,
    kp, up, rb, rp, v1, v2, wx, wy, wzm, wzp, dg, row, gath, staged,
    face_sem, load_sem, send_sem, recv_sem, gsend, grecv, ready,
):
    gx, gy = lax.axis_index("gx"), lax.axis_index("gy")
    xs, ys = [lax.rem(gx + d, ngx) for d in range(ngx)], [lax.rem(gy + d, ngy) for d in range(ngy)]
    barrier = pltpu.get_barrier_semaphore()
    near = [(0, 1), (0, ngy - 1), (1, 0), (ngx - 1, 0), (1, 1), (1, ngy - 1), (ngx - 1, 1), (ngx - 1, ngy - 1)]
    greet = near + [(d, 0) for d in range(2, ngx - 1)] + [(0, d) for d in range(2, ngy - 1)]
    for dx, dy in greet:
        pl.semaphore_signal(
            barrier, inc=1, device_id=(xs[dx], ys[dy]), device_id_type=MESH
        )
    count = ngx * ngy
    loads = []
    for i, (src, dst) in enumerate(((k_hbm, kp), (x0_hbm, up), (rhs_hbm, rb))):
        view = dst.reshape(PLANES, ROWS // 4, 4, 128)
        for q in range(4):
            loads.append(
                pltpu.make_async_copy(
                    src.at[:, :, q * 128 : (q + 1) * 128],
                    view.at[X0:X1, R0 // 4 : R1 // 4, q, :],
                    load_sem.at[i, q],
                )
            )
    face_loads = [
        [
            pltpu.make_async_copy(
                src.at[:, layer : layer + 1, q * 128 : (q + 1) * 128],
                staged.at[i, side, :, q : q + 1, :],
                face_sem.at[i, side, q],
            )
            for side, layer in enumerate((0, 31))
            for q in range(4)
        ]
        for i, src in enumerate((k_hbm, x0_hbm))
    ]
    for copy in face_loads[0] + face_loads[1] + loads[:8]:
        copy.start()
    dirs = directions(gx, gy, ngx, ngy)
    has_low_x, has_high_x, has_low_y, has_high_y = gx > 0, gx < ngx - 1, gy > 0, gy < ngy - 1
    fields = (kp, up, rp, v1, v2)
    zero = jnp.zeros((8, 128), F32)

    for at, inside in ((0, has_low_x), (X1, has_high_x)):

        @pl.when(jnp.logical_not(inside))
        def _():
            def fill(i, c):
                for f in fields:
                    for x in range(at, at + 3):
                        f[x, pl.ds(pl.multiple_of(8 * i, 8), 8), :] = zero
                return c

            lax.fori_loop(0, ROWS // 8, fill, 0)

    for at, inside in ((0, has_low_y), (R1, has_high_y)):

        @pl.when(jnp.logical_not(inside))
        def _():
            def fill(x, c):
                for f in fields:
                    for r in (at, at + 8):
                        f[x, r : r + 8, :] = zero
                return c

            lax.fori_loop(0, PLANES, fill, 0)

    def copy_of(e, f, layers, i):
        sx, sy = dirs[i][:2]
        return pltpu.make_async_remote_copy(
            src_ref=staged.at[e, (sy + 1) // 2] if e < 2 and sx == 0 else piece(f, sx, sy, layers, False),
            dst_ref=piece(f, sx, sy, layers, True),
            send_sem=send_sem.at[e, i], recv_sem=recv_sem.at[e, i],
            device_id={"gx": lax.rem(gx + sx + ngx, ngx), "gy": lax.rem(gy + sy + ngy, ngy)},
            device_id_type=MESH,
        )

    def exchange(e, f, layers, which):
        for i in which:

            @pl.when(dirs[i][2])
            def _():
                copy_of(e, f, layers, i).start()

    def arrived(e, f, layers, which):
        for i in which:

            @pl.when(dirs[i][3])
            def _():
                copy_of(e, f, layers, i).wait_recv()

    def sent(e, f, layers, which):
        for i in which:

            @pl.when(dirs[i][2])
            def _():
                copy_of(e, f, layers, i).wait_send()

    along_y, along_x, corners = (0, 1), (2, 3), (4, 5, 6, 7)
    every_way = corners + along_y + along_x
    faces = along_y + along_x

    with jax.named_scope("load_face"):
        for copy in face_loads[0]:
            copy.wait()
    with jax.named_scope("barrier"):
        pl.semaphore_wait(barrier, len(greet))
        exchange(0, kp, (0, 1), along_y)
        for copy in face_loads[1]:
            copy.wait()
        exchange(1, up, (0, 1), along_y)
    with jax.named_scope("load_k"):
        for copy in loads[:4]:
            copy.wait()
        exchange(0, kp, (0, 1), along_x)
        for copy in loads[8:]:
            copy.start()
        for d in range(1, ngx):
            pl.semaphore_signal(ready, inc=1, device_id=(xs[d], gy), device_id_type=MESH)

    lane = lax.broadcasted_iota(jnp.int32, (8, 128), 1)
    sub = lax.broadcasted_iota(jnp.int32, (8, 128), 0)
    zhi = lax.rem(sub, 4)
    first_lane, last_lane = lane == 0, lane == 127
    z_first = jnp.logical_and(first_lane, zhi == 0)
    z_last = jnp.logical_and(last_lane, zhi == 3)

    def z_up(f, x, r, centre):
        return pltpu.roll(jnp.where(first_lane, f[x, r + 1 : r + 9, :], centre), 127, 1)

    def z_down(f, x, r, centre):
        return pltpu.roll(jnp.where(last_lane, f[x, r - 1 : r + 7, :], centre), 1, 1)

    def weights_x(i, r):
        wx[i, r : r + 8, :] = HALF * (kp[i, r : r + 8, :] + kp[i + 1, r : r + 8, :])

    def weights_y(x, r, n=8):
        wy[x, r : r + n, :] = HALF * (kp[x, r : r + n, :] + kp[x, r + 4 : r + 4 + n, :])

    def weights_z(x, r):
        centre = kp[x, r : r + 8, :]
        above = jnp.where(first_lane, pltpu.roll(centre, 7, 0), centre)
        below = jnp.where(last_lane, pltpu.roll(centre, 1, 0), centre)
        up_w = HALF * (centre + jnp.where(z_last, 0.0, pltpu.roll(above, 127, 1)))
        down_w = HALF * (centre + jnp.where(z_first, 0.0, pltpu.roll(below, 1, 1)))
        dg[x, r : r + 8, :] = up_w + down_w
        wzp[x, r : r + 8, :] = jnp.where(z_last, 0.0, up_w)
        wzm[x, r : r + 8, :] = jnp.where(z_first, 0.0, down_w)

    def add_diagonal(x, r):
        s = slice(r, r + 8)
        dg[x, s, :] = dg[x, s, :] + ((wx[x - 1, s, :] + wx[x, s, :]) + (wy[x, r - 4 : r + 4, :] + wy[x, s, :]))

    def apply(f, x, r):
        s = slice(r, r + 8)
        centre = f[x, s, :]
        out = dg[x, s, :] * centre
        out = out - wx[x - 1, s, :] * f[x - 1, s, :]
        out = out - wx[x, s, :] * f[x + 1, s, :]
        out = out - wy[x, r - 4 : r + 4, :] * f[x, r - 4 : r + 4, :]
        out = out - wy[x, s, :] * f[x, r + 4 : r + 12, :]
        out = out - wzm[x, s, :] * z_down(f, x, r, centre)
        out = out - wzp[x, s, :] * z_up(f, x, r, centre)
        return centre, out

    def chunks(first, last, counts=None):
        return tuple((r, 3 if counts is None else counts) for r in range(R0 + 4 * first, R0 + 4 * last, 8))

    def over(planes, body, carry, unroll=1, start=None):
        def several(planes, carry):
            part = carry if start is None else start
            for x in planes:
                part = body(x, part)
            return part if start is None else tuple(c + p for c, p in zip(carry, part))

        if not isinstance(planes, range):
            return several(planes, carry)
        first, steps = planes.start, len(planes) // unroll
        return lax.fori_loop(
            0, steps, lambda i, carry: several([first + i * unroll + u for u in range(unroll)], carry), carry
        )

    def step(f, w, counted):
        def run(planes, rows, acc, unroll=1):
            def body(x, own):
                for r, layers in rows:
                    centre, out = apply(f, x, r)
                    if f is up:
                        out = rb[x, r : r + 8, :] - SCALE * out
                    inside = True
                    for at, low, high, below, beyond in (
                        (x, X0, X1, has_low_x, has_high_x), (r, R0, R1, has_low_y, has_high_y)
                    ):
                        if isinstance(at, int) and not low <= at < high:
                            inside = False
                            out = jnp.where(below if at < low else beyond, out, 0.0)
                    if w is not None:
                        w[x, r : r + 8, :] = out
                    if not inside or layers == 0:
                        continue
                    terms = (out * out,) if counted == 1 else (centre * out, out * out)
                    if layers < 3:
                        terms = tuple(jnp.where((sub < 4) == (layers == 1), t, 0.0) for t in terms)
                    own = tuple(o + t for o, t in zip(own, terms))
                return own

            return over(planes, body, acc, unroll, (zero,) * counted)

        return run

    own = [r for r, _ in chunks(0, 31)]
    inner = [r for r, _ in chunks(2, 29)]
    ends = (R0, R1 - 8)
    outer = (R0 - 8, R1)

    def own_weights(x, c, with_x=True, diagonal=True):
        for r in own:
            if with_x:
                weights_x(x, r)
            weights_z(x, r)
        for r in own[:-1]:
            weights_y(x, r)
        weights_y(x, R1 - 8, 4)
        if diagonal:
            for r in inner:
                add_diagonal(x, r)
        return c

    with jax.named_scope("weights1"):
        own_weights(X0, 0, diagonal=False)
        over(range(X0 + 1, X0 + 11), own_weights, 0, UW)
        for copy in loads[4:8]:
            copy.wait()
        exchange(1, up, (0, 1), along_x)
        exchange(2, kp, (1, 3), every_way)
    with jax.named_scope("weights2"):
        over(range(X0 + 11, X1 - 1), own_weights, 0, UW)
        own_weights(X1 - 1, 0, with_x=False, diagonal=False)
        for copy in loads[8:]:
            copy.wait()

    residual = step(up, rp, 1)
    m0 = (zero,)
    with jax.named_scope("p1_in"):
        m0 = residual(range(X0 + 1, X1 - 1), chunks(2, 29), m0, U1)
    with jax.named_scope("wait_k"):
        arrived(0, kp, (0, 1), faces)
    with jax.named_scope("edge_weights"):
        for r in own:
            weights_x(X0 - 1, r)
            weights_x(X1 - 1, r)

        def edge(x, c):
            weights_y(x, R0 - 4, 4)
            weights_y(x, R1 - 4, 4)
            for r in ends:
                add_diagonal(x, r)
            return c

        over(range(X0, X1), edge, 0, UY)
        for x in (X0, X1 - 1):
            for r in inner:
                add_diagonal(x, r)
    with jax.named_scope("p1_waitx"):
        arrived(1, up, (0, 1), along_x)
    with jax.named_scope("p1_ringx"):
        m0 = residual((X0, X1 - 1), chunks(2, 29), m0)
    high_last = lax.rem(gy, 4) == 3
    sides = (((0,), (5, 7), chunks(0, 1)), ((1,), (4, 6), chunks(30, 31)))

    def residual_strips(order):
        def run(m0):
            for side in order:
                with jax.named_scope("p1_waity%d" % side):
                    arrived(1, up, (0, 1), sides[side][0])
                with jax.named_scope("p1_ringy%d" % side):
                    m0 = residual(tuple(range(X0, X1)), sides[side][2], m0)
                    exchange(3, rp, (0, 3), sides[side][1] + (1 - side,))
            return m0

        return run

    m0 = lax.cond(high_last, residual_strips((0, 1)), residual_strips((1, 0)), m0)
    exchange(3, rp, (0, 3), along_x)

    powers = (step(rp, v1, 2), step(v1, v2, 2), step(v2, None, 2))
    rows = (chunks(1, 30), chunks(2, 29), chunks(3, 28))
    acc = [(zero, zero)] * 3
    depth = (1, 2, 4)
    for n in range(3):
        with jax.named_scope("p2_in%d" % n):
            acc[n] = powers[n](range(X0 + depth[n], X1 - depth[n]), rows[n], acc[n], (U1, U2, U3)[n])
    with jax.named_scope("wait_k2"):
        arrived(2, kp, (1, 3), every_way)
    with jax.named_scope("halo_weights"):
        beside = (X0 - 2, X0 - 1, X1, X1 + 1)
        for i in (X0 - 3, X0 - 2, X1, X1 + 1):
            for r in own:
                weights_x(i, r)
        for x in beside:
            for r in own:
                weights_z(x, r)
                weights_y(x, r)
            weights_y(x, R0 - 4, 4)
            for r in own:
                add_diagonal(x, r)

        def halo(x, c, with_x=True):
            weights_y(x, R0 - 12, 8)
            weights_y(x, R1, 8)
            for r in outer:
                weights_x(x, r)
                weights_z(x, r)
                add_diagonal(x, r)
            return c

        for r in outer:
            weights_x(X0 - 2, r)
        halo(X0 - 1, 0)
        over(range(X0, X1), halo, 0, UY)
        halo(X1, 0)
    with jax.named_scope("p2_waitx"):
        arrived(3, rp, (0, 3), along_x)
    with jax.named_scope("p2_ringx"):
        for n in range(3):
            low, high = X0 - 2 + n, X1 + 2 - n
            acc[n] = powers[n](tuple(range(low, X0 + depth[n])) + tuple(range(X1 - depth[n], high)), rows[n], acc[n])
    strips = (
        ((0, 4, 6), chunks(0, 1, 1), chunks(-2, -1, 0), chunks(0, 1), chunks(0, 1) + chunks(2, 3, 1)),
        ((1, 5, 7), chunks(30, 31, 2), chunks(32, 33, 0), chunks(30, 31), chunks(28, 29, 2) + chunks(30, 31)),
    )

    def power_strips(order):
        def run(acc):
            acc = list(acc)
            for side in order:
                ways, line, halos, line1, line2 = strips[side]
                with jax.named_scope("p2_waity%d" % side):
                    arrived(3, rp, (0, 3), ways)
                with jax.named_scope("p2_ringy%d" % side):
                    acc[0] = powers[0](beside, line, acc[0])
                    acc[0] = powers[0]((X0 - 1, X1), halos, acc[0])
                    acc[0] = powers[0](tuple(range(X0, X1)), line + halos, acc[0])
                    acc[1] = powers[1]((X0 - 1, X1), line1, acc[1])
                    acc[1] = powers[1](tuple(range(X0, X1)), line1 + halos, acc[1])
                    acc[2] = powers[2](tuple(range(X0, X1)), line2, acc[2])
            return tuple(acc)

        return run

    acc = lax.cond(high_last, power_strips((0, 1)), power_strips((1, 0)), tuple(acc))
    (m1, m2), (m3, m4), (m5, m6) = acc
    m0 = m0[0]
    moments = [m0, m1, m2, m3, m4, m5, m6]

    with jax.named_scope("moments"):
        stacked = zero
        for k, m in enumerate(moments):
            stacked = jnp.where(sub == k, jnp.sum(m, axis=0, keepdims=True), stacked)
        high, low = split_sum(stacked, 1)
        mine = jnp.sum(jnp.where(lane == sub, high, jnp.where(lane == sub + 8, low, 0.0)), axis=0, keepdims=True)
    place = gx * ngy + gy
    row[...] = mine
    gath[pl.ds(place, 1), :] = mine
    pl.semaphore_wait(ready, ngx - 1)
    with jax.named_scope("gsend"):
        for dx, dy in far_first(ngx, ngy):
            pltpu.make_async_remote_copy(
                src_ref=row, dst_ref=gath.at[pl.ds(place, 1), :], send_sem=gsend, recv_sem=grecv,
                device_id=(xs[dx], ys[dy]), device_id_type=MESH,
            ).start()
    every = pltpu.make_async_remote_copy(
        src_ref=gath.at[0 : count - 1, :], dst_ref=gath.at[0 : count - 1, :], send_sem=gsend, recv_sem=grecv,
        device_id=(gx, gy), device_id_type=MESH,
    )
    with jax.named_scope("gwait"):
        every.wait_recv()
    with jax.named_scope("solve"):
        high, low = split_sum(gath[...], 0)
        lane1 = lax.broadcasted_iota(jnp.int32, (1, 128), 1)

        def pick(v, k):
            return jnp.sum(jnp.where(lane1 == k, v, 0.0), axis=1, keepdims=True)

        m = [renorm(pick(high, k), pick(low, k) + pick(high + low, k + 8)) for k in range(7)]
        (y1, y2, y3), rest = normal_equations(m)
        est_ref[...] = jnp.broadcast_to(jnp.sqrt(jnp.maximum(rest, 0.0)), (1, 128))
        y1, y2, y3 = (jnp.broadcast_to(y, (8, 128)) for y in (y1, y2, y3))

    def combine(x, c):
        for y in range(0, 32, 8):
            for q in range(4):
                s = pl.ds(R0 + 4 * y + q, 8, stride=4)
                sol_ref[x - X0, y : y + 8, q * 128 : (q + 1) * 128] = up[x, s, :] + (
                    y1 * rp[x, s, :] + (y2 * v1[x, s, :] + y3 * v2[x, s, :])
                )
        return c

    with jax.named_scope("final"):
        over(range(X0, X1), combine, 0, 2)
    every.wait_send()
    sent(0, kp, (0, 1), faces)
    sent(1, up, (0, 1), faces)
    sent(2, kp, (1, 3), every_way)
    sent(3, rp, (0, 3), every_way)


def local(ngx, ngy, right_side, start_guess, conductivity):
    field = pltpu.VMEM((PLANES, ROWS, 128), F32)
    sem = pltpu.SemaphoreType
    sol, est = pl.pallas_call(
        functools.partial(kernel, ngx, ngy),
        out_shape=(jax.ShapeDtypeStruct((32, 32, 512), F32), jax.ShapeDtypeStruct((1, 128), F32)),
        in_specs=[pl.BlockSpec(memory_space=pltpu.HBM)] * 3,
        out_specs=(pl.BlockSpec(memory_space=pltpu.VMEM), pl.BlockSpec(memory_space=pltpu.VMEM)),
        scratch_shapes=[field] * 11 + [
            pltpu.VMEM((1, 128), F32),
            pltpu.VMEM((ngx * ngy, 128), F32),
            pltpu.VMEM((2, 2, 32, 4, 128), F32),
            sem.DMA((2, 2, 4)), sem.DMA((3, 4)), sem.DMA((4, 8)), sem.DMA((4, 8)), sem.DMA, sem.DMA, sem.REGULAR,
        ],
        compiler_params=pltpu.CompilerParams(
            collective_id=0, has_side_effects=True, vmem_limit_bytes=50 * 2**20
        ),
    )(right_side, start_guess, conductivity)
    return sol, est[0, 0]


def solution(mesh):
    return jax.shard_map(
        functools.partial(local, mesh.shape["gx"], mesh.shape["gy"]),
        mesh=mesh,
        in_specs=(P("gx", "gy", None),) * 3,
        out_specs=(P("gx", "gy", None), P()),
        check_vma=False,
    )
```

```python
import functools

import jax
import jax.numpy as jnp
from jax import lax
from jax.experimental import pallas as pl
from jax.experimental.pallas import tpu as pltpu
from jax.sharding import PartitionSpec as P

MESH = pl.DeviceIdType.MESH
F32 = jnp.float32
SCALE = 64.0
HALF = 0.5 / SCALE
X0, X1 = 3, 35
R0, R1 = 16, 144
PLANES, ROWS = 38, 160
UW, U1, U2, U3, UY = 5, 5, 4, 4, 8


def renorm(a, b):
    s = a + b
    return s, b - (s - a)


def two_sum(a, b):
    s = a + b
    t = s - a
    return s, (a - (s - t)) + (b - t)


def split(a):
    t = 4097.0 * a
    high = t - (t - a)
    return high, a - high


def two_prod(a, b):
    p = a * b
    (ah, al), (bh, bl) = split(a), split(b)
    return p, ((ah * bh - p) + ah * bl + al * bh) + al * bl


def add(a, b):
    s, e = two_sum(a[0], b[0])
    return renorm(s, e + (a[1] + b[1]))


def sub(a, b):
    return add(a, (-b[0], -b[1]))


def mul(a, b):
    p, e = two_prod(a[0], b[0])
    return renorm(p, e + (a[0] * b[1] + a[1] * b[0]))


def div(a, b):
    q = a[0] / b[0]
    p, e = two_prod(q, b[0])
    return renorm(q, (((a[0] - p) - e) + (a[1] - q * b[1])) / b[0])


def split_sum(v, axis):
    bound = 2.0 * jnp.sum(jnp.abs(v), axis=axis, keepdims=True)
    upper = (v + bound) - bound
    return jnp.sum(upper, axis=axis, keepdims=True), jnp.sum(v - upper, axis=axis, keepdims=True)


def normal_equations(m):
    l21, l31 = div(m[3], m[2]), div(m[4], m[2])
    d2 = sub(m[4], mul(l21, m[3]))
    e2 = sub(m[5], mul(l21, m[4]))
    l32 = div(e2, d2)
    d3 = sub(sub(m[6], mul(l31, m[4])), mul(l32, e2))
    c1 = m[1]
    c2 = sub(m[2], mul(l21, c1))
    c3 = sub(sub(m[3], mul(l31, c1)), mul(l32, c2))
    q1, q2, q3 = div(c1, m[2]), div(c2, d2), div(c3, d3)
    y3 = q3
    y2 = sub(q2, mul(l32, y3))
    y1 = sub(sub(q1, mul(l21, y2)), mul(l31, y3))
    rest = sub(sub(sub(m[0], mul(c1, q1)), mul(c2, q2)), mul(c3, q3))
    return tuple(y[0] / SCALE for y in (y1, y2, y3)), rest[0]


def directions(gx, gy, ngx, ngy, reach=1):
    out = []
    for sx, sy in ((0, 1), (0, -1), (1, 0), (-1, 0), (1, 1), (1, -1), (-1, 1), (-1, -1)):
        to, come = [], []
        for step, at, n in ((sx, gx, ngx), (sy, gy, ngy)):
            if step:
                low, high = at >= reach, at < n - reach
                to.append(high if step > 0 else low)
                come.append(low if step > 0 else high)
        both = (lambda c: c[0]) if len(to) == 1 else (lambda c: jnp.logical_and(*c))
        out.append((sx, sy, both(to), both(come)))
    return out


def far_first(ngx, ngy):
    def ring(d):
        return min(d % 4, -d % 4)

    offsets = [(dx, dy) for dx in range(ngx) for dy in range(ngy) if dx or dy]
    return sorted(offsets, key=lambda o: -(ring(o[0] // 2) + ring(o[1] // 4) + ring(o[1] % 4)))


def extent(step, low, high, near, far, outside):
    if step == 0:
        return slice(low, high)
    if outside:
        return slice(low - far, low - near) if step > 0 else slice(high + near, high + far)
    return slice(high - far, high - near) if step > 0 else slice(low + near, low + far)


def piece(ref, sx, sy, layers, outside):
    near, far = (0, 2) if sx and sy else layers
    return ref.at[extent(sx, X0, X1, near, far, outside), extent(sy, R0, R1, 4 * near, 4 * far, outside), :]


def kernel(
    ngx, ngy,
    rhs_hbm, x0_hbm, k_hbm, sol_ref, est_ref,
    kp, up, rb, rp, v1, v2, wx, wy, wzm, wzp, dg, row, gath, staged,
    face_sem, load_sem, send_sem, recv_sem, gsend, grecv, ready,
):
    gx, gy = lax.axis_index("gx"), lax.axis_index("gy")
    xs, ys = [lax.rem(gx + d, ngx) for d in range(ngx)], [lax.rem(gy + d, ngy) for d in range(ngy)]
    barrier = pltpu.get_barrier_semaphore()
    def greet(sem, reach):
        for sx, sy, to, _ in directions(gx, gy, ngx, ngy, reach):

            @pl.when(to)
            def _():
                pl.semaphore_signal(
                    sem, inc=1, device_id=(xs[sx * reach % ngx], ys[sy * reach % ngy]), device_id_type=MESH
                )

    def greeted(sem, reach):
        senders = [jnp.where(come, 1, 0) for _, _, _, come in directions(gx, gy, ngx, ngy, reach)]
        pl.semaphore_wait(sem, sum(senders[1:], senders[0]))

    greet(barrier, 1)
    count = ngx * ngy
    loads = []
    for i, (src, dst) in enumerate(((k_hbm, kp), (x0_hbm, up), (rhs_hbm, rb))):
        view = dst.reshape(PLANES, ROWS // 4, 4, 128)
        for q in range(4):
            loads.append(
                pltpu.make_async_copy(
                    src.at[:, :, q * 128 : (q + 1) * 128],
                    view.at[X0:X1, R0 // 4 : R1 // 4, q, :],
                    load_sem.at[i, q],
                )
            )
    face_loads = [
        [
            pltpu.make_async_copy(
                src.at[:, layer : layer + 1, q * 128 : (q + 1) * 128],
                staged.at[i, side, :, q : q + 1, :],
                face_sem.at[i, side, q],
            )
            for side, layer in enumerate((0, 31))
            for q in range(4)
        ]
        for i, src in enumerate((k_hbm, x0_hbm))
    ]
    for copy in face_loads[0] + face_loads[1] + loads[:8]:
        copy.start()
    dirs = directions(gx, gy, ngx, ngy)
    has_low_x, has_high_x, has_low_y, has_high_y = gx > 0, gx < ngx - 1, gy > 0, gy < ngy - 1
    fields = (kp, up, rp, v1, v2)
    zero = jnp.zeros((8, 128), F32)

    def copy_of(e, f, layers, i):
        sx, sy = dirs[i][:2]
        return pltpu.make_async_remote_copy(
            src_ref=staged.at[e, (sy + 1) // 2] if e < 2 and sx == 0 else piece(f, sx, sy, layers, False),
            dst_ref=piece(f, sx, sy, layers, True),
            send_sem=send_sem.at[e, i], recv_sem=recv_sem.at[e, i],
            device_id={"gx": lax.rem(gx + sx + ngx, ngx), "gy": lax.rem(gy + sy + ngy, ngy)},
            device_id_type=MESH,
        )

    def exchange(e, f, layers, which):
        for i in which:

            @pl.when(dirs[i][2])
            def _():
                copy_of(e, f, layers, i).start()

    def arrived(e, f, layers, which):
        for i in which:

            @pl.when(dirs[i][3])
            def _():
                copy_of(e, f, layers, i).wait_recv()

    def sent(e, f, layers, which):
        for i in which:

            @pl.when(dirs[i][2])
            def _():
                copy_of(e, f, layers, i).wait_send()

    along_y, along_x, corners = (0, 1), (2, 3), (4, 5, 6, 7)
    every_way = corners + along_y + along_x
    faces = along_y + along_x

    with jax.named_scope("load_face"):
        for copy in face_loads[0]:
            copy.wait()
    with jax.named_scope("barrier"):
        greeted(barrier, 1)
        exchange(0, kp, (0, 1), along_y)
        for copy in face_loads[1]:
            copy.wait()
        exchange(1, up, (0, 1), along_y)
    with jax.named_scope("load_k"):
        for copy in loads[:4]:
            copy.wait()
        exchange(0, kp, (0, 1), along_x)
        for copy in loads[8:]:
            copy.start()
        greet(ready.at[0], 1)

    for at, inside in ((0, has_low_x), (X1, has_high_x)):

        @pl.when(jnp.logical_not(inside))
        def _():
            def fill(i, c):
                for f in fields:
                    for x in range(at, at + 3):
                        f[x, pl.ds(pl.multiple_of(8 * i, 8), 8), :] = zero
                return c

            lax.fori_loop(0, ROWS // 8, fill, 0)

    for at, inside in ((0, has_low_y), (R1, has_high_y)):

        @pl.when(jnp.logical_not(inside))
        def _():
            def fill(x, c):
                for f in fields:
                    for r in (at, at + 8):
                        f[x, r : r + 8, :] = zero
                return c

            lax.fori_loop(0, PLANES, fill, 0)

    lane = lax.broadcasted_iota(jnp.int32, (8, 128), 1)
    sub = lax.broadcasted_iota(jnp.int32, (8, 128), 0)
    zhi = lax.rem(sub, 4)
    first_lane, last_lane = lane == 0, lane == 127
    z_first = jnp.logical_and(first_lane, zhi == 0)
    z_last = jnp.logical_and(last_lane, zhi == 3)

    def z_up(f, x, r, centre):
        return pltpu.roll(jnp.where(first_lane, f[x, r + 1 : r + 9, :], centre), 127, 1)

    def z_down(f, x, r, centre):
        return pltpu.roll(jnp.where(last_lane, f[x, r - 1 : r + 7, :], centre), 1, 1)

    def weights_x(i, r):
        wx[i, r : r + 8, :] = HALF * (kp[i, r : r + 8, :] + kp[i + 1, r : r + 8, :])

    def weights_y(x, r, n=8):
        wy[x, r : r + n, :] = HALF * (kp[x, r : r + n, :] + kp[x, r + 4 : r + 4 + n, :])

    def weights_z(x, r):
        centre = kp[x, r : r + 8, :]
        above = jnp.where(first_lane, pltpu.roll(centre, 7, 0), centre)
        below = jnp.where(last_lane, pltpu.roll(centre, 1, 0), centre)
        up_w = HALF * (centre + jnp.where(z_last, 0.0, pltpu.roll(above, 127, 1)))
        down_w = HALF * (centre + jnp.where(z_first, 0.0, pltpu.roll(below, 1, 1)))
        dg[x, r : r + 8, :] = up_w + down_w
        wzp[x, r : r + 8, :] = jnp.where(z_last, 0.0, up_w)
        wzm[x, r : r + 8, :] = jnp.where(z_first, 0.0, down_w)

    def add_diagonal(x, r):
        s = slice(r, r + 8)
        dg[x, s, :] = dg[x, s, :] + ((wx[x - 1, s, :] + wx[x, s, :]) + (wy[x, r - 4 : r + 4, :] + wy[x, s, :]))

    def apply(f, x, r):
        s = slice(r, r + 8)
        centre = f[x, s, :]
        out = dg[x, s, :] * centre
        out = out - wx[x - 1, s, :] * f[x - 1, s, :]
        out = out - wx[x, s, :] * f[x + 1, s, :]
        out = out - wy[x, r - 4 : r + 4, :] * f[x, r - 4 : r + 4, :]
        out = out - wy[x, s, :] * f[x, r + 4 : r + 12, :]
        out = out - wzm[x, s, :] * z_down(f, x, r, centre)
        out = out - wzp[x, s, :] * z_up(f, x, r, centre)
        return centre, out

    def chunks(first, last, counts=None):
        return tuple((r, 3 if counts is None else counts) for r in range(R0 + 4 * first, R0 + 4 * last, 8))

    def over(planes, body, carry, unroll=1, start=None):
        def several(planes, carry):
            part = carry if start is None else start
            for x in planes:
                part = body(x, part)
            return part if start is None else tuple(c + p for c, p in zip(carry, part))

        if not isinstance(planes, range):
            return several(planes, carry)
        first, steps = planes.start, len(planes) // unroll
        return lax.fori_loop(
            0, steps, lambda i, carry: several([first + i * unroll + u for u in range(unroll)], carry), carry
        )

    def step(f, w, counted):
        def run(planes, rows, acc, unroll=1):
            def body(x, own):
                for r, layers in rows:
                    centre, out = apply(f, x, r)
                    if f is up:
                        out = rb[x, r : r + 8, :] - SCALE * out
                    inside = True
                    for at, low, high, below, beyond in (
                        (x, X0, X1, has_low_x, has_high_x), (r, R0, R1, has_low_y, has_high_y)
                    ):
                        if isinstance(at, int) and not low <= at < high:
                            inside = False
                            out = jnp.where(below if at < low else beyond, out, 0.0)
                    if w is not None:
                        w[x, r : r + 8, :] = out
                    if not inside or layers == 0:
                        continue
                    terms = (out * out,) if counted == 1 else (centre * out, out * out)
                    if layers < 3:
                        terms = tuple(jnp.where((sub < 4) == (layers == 1), t, 0.0) for t in terms)
                    own = tuple(o + t for o, t in zip(own, terms))
                return own

            return over(planes, body, acc, unroll, (zero,) * counted)

        return run

    own = [r for r, _ in chunks(0, 31)]
    inner = [r for r, _ in chunks(2, 29)]
    ends = (R0, R1 - 8)
    outer = (R0 - 8, R1)

    def own_weights(x, c, with_x=True, diagonal=True):
        for r in own:
            if with_x:
                weights_x(x, r)
            weights_z(x, r)
        for r in own[:-1]:
            weights_y(x, r)
        weights_y(x, R1 - 8, 4)
        if diagonal:
            for r in inner:
                add_diagonal(x, r)
        return c

    with jax.named_scope("weights1"):
        own_weights(X0, 0, diagonal=False)
        over(range(X0 + 1, X0 + 11), own_weights, 0, UW)
        for copy in loads[4:8]:
            copy.wait()
        exchange(1, up, (0, 1), along_x)
        exchange(2, kp, (1, 3), every_way)
    with jax.named_scope("weights2"):
        over(range(X0 + 11, X1 - 1), own_weights, 0, UW)
        own_weights(X1 - 1, 0, with_x=False, diagonal=False)
        for copy in loads[8:]:
            copy.wait()
        greeted(ready.at[0], 1)
        greet(ready.at[1], 2)

    residual = step(up, rp, 1)
    m0 = (zero,)
    with jax.named_scope("p1_in"):
        m0 = residual(range(X0 + 1, X1 - 1), chunks(2, 29), m0, U1)
    with jax.named_scope("wait_k"):
        arrived(0, kp, (0, 1), faces)
    with jax.named_scope("edge_weights"):
        for r in own:
            weights_x(X0 - 1, r)
            weights_x(X1 - 1, r)

        def edge(x, c):
            weights_y(x, R0 - 4, 4)
            weights_y(x, R1 - 4, 4)
            for r in ends:
                add_diagonal(x, r)
            return c

        over(range(X0, X1), edge, 0, UY)
        for x in (X0, X1 - 1):
            for r in inner:
                add_diagonal(x, r)
    with jax.named_scope("p1_waitx"):
        arrived(1, up, (0, 1), along_x)
    with jax.named_scope("p1_ringx"):
        m0 = residual((X0, X1 - 1), chunks(2, 29), m0)
    high_last = lax.rem(gy, 4) == 3
    sides = (((0,), (5, 7), chunks(0, 1)), ((1,), (4, 6), chunks(30, 31)))

    def residual_strips(order):
        def run(m0):
            for side in order:
                with jax.named_scope("p1_waity%d" % side):
                    arrived(1, up, (0, 1), sides[side][0])
                with jax.named_scope("p1_ringy%d" % side):
                    m0 = residual(tuple(range(X0, X1)), sides[side][2], m0)
                    exchange(3, rp, (0, 3), sides[side][1] + (1 - side,))
            return m0

        return run

    m0 = lax.cond(high_last, residual_strips((0, 1)), residual_strips((1, 0)), m0)
    exchange(3, rp, (0, 3), along_x)
    greeted(ready.at[1], 2)
    greet(ready.at[2], 4)

    powers = (step(rp, v1, 2), step(v1, v2, 2), step(v2, None, 2))
    rows = (chunks(1, 30), chunks(2, 29), chunks(3, 28))
    acc = [(zero, zero)] * 3
    depth = (1, 2, 4)
    for n in range(3):
        with jax.named_scope("p2_in%d" % n):
            acc[n] = powers[n](range(X0 + depth[n], X1 - depth[n]), rows[n], acc[n], (U1, U2, U3)[n])
    greeted(ready.at[2], 4)
    greet(ready.at[3], 8)
    with jax.named_scope("wait_k2"):
        arrived(2, kp, (1, 3), every_way)
    with jax.named_scope("halo_weights"):
        beside = (X0 - 2, X0 - 1, X1, X1 + 1)
        for i in (X0 - 3, X0 - 2, X1, X1 + 1):
            for r in own:
                weights_x(i, r)
        for x in beside:
            for r in own:
                weights_z(x, r)
                weights_y(x, r)
            weights_y(x, R0 - 4, 4)
            for r in own:
                add_diagonal(x, r)

        def halo(x, c, with_x=True):
            weights_y(x, R0 - 12, 8)
            weights_y(x, R1, 8)
            for r in outer:
                weights_x(x, r)
                weights_z(x, r)
                add_diagonal(x, r)
            return c

        for r in outer:
            weights_x(X0 - 2, r)
        halo(X0 - 1, 0)
        over(range(X0, X1), halo, 0, UY)
        halo(X1, 0)
    with jax.named_scope("p2_waitx"):
        arrived(3, rp, (0, 3), along_x)
    with jax.named_scope("p2_ringx"):
        for n in range(3):
            low, high = X0 - 2 + n, X1 + 2 - n
            acc[n] = powers[n](tuple(range(low, X0 + depth[n])) + tuple(range(X1 - depth[n], high)), rows[n], acc[n])
    strips = (
        ((0, 4, 6), chunks(0, 1, 1), chunks(-2, -1, 0), chunks(0, 1), chunks(0, 1) + chunks(2, 3, 1)),
        ((1, 5, 7), chunks(30, 31, 2), chunks(32, 33, 0), chunks(30, 31), chunks(28, 29, 2) + chunks(30, 31)),
    )

    def power_strips(order):
        def run(acc):
            acc = list(acc)
            for side in order:
                ways, line, halos, line1, line2 = strips[side]
                with jax.named_scope("p2_waity%d" % side):
                    arrived(3, rp, (0, 3), ways)
                with jax.named_scope("p2_ringy%d" % side):
                    acc[0] = powers[0](beside, line, acc[0])
                    acc[0] = powers[0]((X0 - 1, X1), halos, acc[0])
                    acc[0] = powers[0](tuple(range(X0, X1)), line + halos, acc[0])
                    acc[1] = powers[1]((X0 - 1, X1), line1, acc[1])
                    acc[1] = powers[1](tuple(range(X0, X1)), line1 + halos, acc[1])
                    acc[2] = powers[2](tuple(range(X0, X1)), line2, acc[2])
            return tuple(acc)

        return run

    acc = lax.cond(high_last, power_strips((0, 1)), power_strips((1, 0)), tuple(acc))
    (m1, m2), (m3, m4), (m5, m6) = acc
    m0 = m0[0]
    moments = [m0, m1, m2, m3, m4, m5, m6]

    with jax.named_scope("moments"):
        stacked = zero
        for k, m in enumerate(moments):
            stacked = jnp.where(sub == k, jnp.sum(m, axis=0, keepdims=True), stacked)
        high, low = split_sum(stacked, 1)
        mine = jnp.sum(jnp.where(lane == sub, high, jnp.where(lane == sub + 8, low, 0.0)), axis=0, keepdims=True)
    place = gx * ngy + gy
    row[...] = mine
    gath[pl.ds(place, 1), :] = mine
    greeted(ready.at[3], 8)
    with jax.named_scope("gsend"):
        for dx, dy in far_first(ngx, ngy):
            pltpu.make_async_remote_copy(
                src_ref=row, dst_ref=gath.at[pl.ds(place, 1), :], send_sem=gsend, recv_sem=grecv,
                device_id=(xs[dx], ys[dy]), device_id_type=MESH,
            ).start()
    every = pltpu.make_async_remote_copy(
        src_ref=gath.at[0 : count - 1, :], dst_ref=gath.at[0 : count - 1, :], send_sem=gsend, recv_sem=grecv,
        device_id=(gx, gy), device_id_type=MESH,
    )
    with jax.named_scope("gwait"):
        every.wait_recv()
    with jax.named_scope("solve"):
        high, low = split_sum(gath[...], 0)
        lane1 = lax.broadcasted_iota(jnp.int32, (1, 128), 1)

        def pick(v, k):
            return jnp.sum(jnp.where(lane1 == k, v, 0.0), axis=1, keepdims=True)

        m = [renorm(pick(high, k), pick(low, k) + pick(high + low, k + 8)) for k in range(7)]
        (y1, y2, y3), rest = normal_equations(m)
        est_ref[...] = jnp.broadcast_to(jnp.sqrt(jnp.maximum(rest, 0.0)), (1, 128))
        y1, y2, y3 = (jnp.broadcast_to(y, (8, 128)) for y in (y1, y2, y3))

    def combine(x, c):
        for y in range(0, 32, 8):
            for q in range(4):
                s = pl.ds(R0 + 4 * y + q, 8, stride=4)
                sol_ref[x - X0, y : y + 8, q * 128 : (q + 1) * 128] = up[x, s, :] + (
                    y1 * rp[x, s, :] + (y2 * v1[x, s, :] + y3 * v2[x, s, :])
                )
        return c

    with jax.named_scope("final"):
        over(range(X0, X1), combine, 0, 2)
    every.wait_send()
    sent(0, kp, (0, 1), faces)
    sent(1, up, (0, 1), faces)
    sent(2, kp, (1, 3), every_way)
    sent(3, rp, (0, 3), every_way)


def local(ngx, ngy, right_side, start_guess, conductivity):
    field = pltpu.VMEM((PLANES, ROWS, 128), F32)
    sem = pltpu.SemaphoreType
    sol, est = pl.pallas_call(
        functools.partial(kernel, ngx, ngy),
        out_shape=(jax.ShapeDtypeStruct((32, 32, 512), F32), jax.ShapeDtypeStruct((1, 128), F32)),
        in_specs=[pl.BlockSpec(memory_space=pltpu.HBM)] * 3,
        out_specs=(pl.BlockSpec(memory_space=pltpu.VMEM), pl.BlockSpec(memory_space=pltpu.VMEM)),
        scratch_shapes=[field] * 11 + [
            pltpu.VMEM((1, 128), F32),
            pltpu.VMEM((ngx * ngy, 128), F32),
            pltpu.VMEM((2, 2, 32, 4, 128), F32),
            sem.DMA((2, 2, 4)), sem.DMA((3, 4)), sem.DMA((4, 8)), sem.DMA((4, 8)), sem.DMA, sem.DMA, sem.REGULAR((4,)),
        ],
        compiler_params=pltpu.CompilerParams(
            collective_id=0, has_side_effects=True, vmem_limit_bytes=50 * 2**20
        ),
    )(right_side, start_guess, conductivity)
    return sol, est[0, 0]


def solution(mesh):
    return jax.shard_map(
        functools.partial(local, mesh.shape["gx"], mesh.shape["gy"]),
        mesh=mesh,
        in_specs=(P("gx", "gy", None),) * 3,
        out_specs=(P("gx", "gy", None), P()),
        check_vma=False,
    )
```
